256 devices in a mesh: rep: 2 (over y), seq: 16 (over z), section: 2 (over core), head: 4 (over x).
Axes of the slice: x: 4, y: 2, z: 16, core: 2. Of those that a mesh axis runs over, the one named last changes fastest.
The devices are a block of a 4x16x16 slice.
Arguments:
- hidden: bfloat16 [6, 1024, 2048], P('rep', 'seq'), parts along dimension 0, may hold values from -6 to 6
- lengths: int32 [6], P('rep'), parts along dimension 0, may hold values from 1 to 1024, 2304 in all
- attn_gain: float32 [2, 2048], P('section'), may hold values from 0.1 to 1.9
- w_query: bfloat16 [2, 2048, 2048], P('section', None, 'head'), may hold values from -2 to 2
- w_latent: bfloat16 [2, 2048, 512], P('section'), may hold values from -0.125 to 0.125
- latent_gain: float32 [2, 512], P('section'), may hold values from 0.1 to 1.9
- w_key: bfloat16 [2, 512, 2048], P('section', None, 'head'), may hold values from -0.25 to 0.25
- w_value: bfloat16 [2, 512, 2048], P('section', None, 'head'), may hold values from -0.25 to 0.25
- w_out: bfloat16 [2, 2048, 2048], P('section', 'head'), may hold values from -0.125 to 0.125
Outputs:
- final: float32 [6, 1024, 2048], P('rep', ('seq', 'head'), 'section'), parts along dimension 0
- latents: float32 [2, 6, 1024, 512], P('section', 'rep', 'seq'), parts along dimension 1
The draws below stay inside these ranges and needn't reach their ends.
There are 2 independent parts, one for each index of `rep`. The reference program is written for one: setup_inputs(seed, part) draws one part's arguments, and reference() takes and returns one part's arrays. A program takes and returns all parts, laid end to end along the dimension named above; an argument that names none is the same for every part. Nothing has to cross between parts.
Inputs may be any that keep to these rules, and one draw needn't show every extreme that they name: lengths sum to 2304 and one block holds exactly 1024; the live tokens of a block are its first slots.
All inputs are finite; a program needn't handle non-finite values.
Results may differ from the reference program's by a relative error of at most 0.015.
The reference program's roundings to bfloat16 on the way (of `normed`, `query`, `latent`, `absorbed`, `rounded`, `context` and `attn`) count: a program that leaves them out, or rounds other values in their place, can miss the bound.
Values may be sent and summed in bfloat16 or wider, within the bound.
A program may use at most 128 MiB of HBM per device.

```python
import math
import jax
import jax.numpy as jnp
import numpy as np
from jax import lax

D = 2048
HEADS = 16
HD = 128
R = 512
GROUPS = 3
TOKC = 1024
LAYERS = 2


def draw_w_query(key, part):
    full_shape = (LAYERS, D, HEADS * HD)
    entries = jax.random.truncated_normal(key, -6.0, 6.0, full_shape, jnp.float32) * D ** (-0.5)
    return entries.astype(jnp.bfloat16)


def block_levels(stream_key, dims, cuts, smallest, top_value):
    factor_of = 1.0
    for axis_at, parts in cuts:
        draws = jax.random.uniform(jax.random.fold_in(jax.random.fold_in(stream_key, 6), axis_at), (parts,), jnp.float32, smallest / len(cuts), top_value / len(cuts))
        factor_of = factor_of * jnp.repeat(jnp.exp(draws), dims[axis_at] // parts).reshape((-1,) + (1,) * (len(dims) - 1 - axis_at))
    return factor_of


def length_profile(count, total, most, lean):
    loads = [(1 << 20) // math.isqrt(rank ** lean) + 1 for rank in range(2, count + 1)]
    spare, counts = total - most - (count - 1), [1] * (count - 1)
    while spare > 0:
        candidates = [i for i in range(count - 1) if counts[i] < most]
        pool, left = sum([loads[i] for i in candidates]), spare
        for i in candidates:
            more = min(most - counts[i], max(1, left * loads[i] // pool), spare)
            counts[i] = counts[i] + more
            spare = spare - more
    return np.array([most] + counts)


def uneven_parts(stream_key, number_of, total, bound, slope):
    if number_of == 2:
        one = jax.random.randint(stream_key, (), max(1, total - bound), min(bound, total - 1) + 1)
        return jnp.stack([one, total - one])
    tallies = jnp.asarray(length_profile(number_of, total, bound, slope), jnp.int32)
    twos = (number_of - 1) // 2
    source_of, receiver = tallies[1:1 + 2 * twos:2], tallies[2:2 + 2 * twos:2]
    slack = jnp.minimum(source_of - 1, bound - receiver)
    shifted = jax.random.randint(jax.random.fold_in(stream_key, 1), (twos,), 0, 1 << 20) % (slack + 1)
    tallies = tallies.at[1:1 + 2 * twos:2].set(source_of - shifted).at[2:2 + 2 * twos:2].set(receiver + shifted)
    return tallies[jax.random.permutation(jax.random.fold_in(stream_key, 2), number_of)]


def bell_draw(rng, extent, scale, bound, cuts=(), kind=jnp.bfloat16):
    values = scale * jax.random.normal(rng, extent, jnp.float32)
    if cuts:
        values = values * block_levels(rng, extent, cuts, -0.22, 0.18)
    return jnp.clip(values, -bound, bound).astype(kind)


def setup_inputs(seed: int = 0, part: int = 0) -> dict:
    streams_of = jax.random.split(jax.random.key(seed), 10)
    part_splits = jax.random.split(jax.random.fold_in(streams_of[9], part), 10)
    return {
        "hidden": bell_draw(part_splits[0], (GROUPS, TOKC, D), 1.0, 6.0, ((1, 16),)),
        "lengths": uneven_parts(part_splits[1], GROUPS, 3 * GROUPS * TOKC // 4, TOKC, 2).astype(jnp.int32),
        "attn_gain": jnp.clip(1.0 + 0.18 * jax.random.normal(streams_of[2], (LAYERS, D), jnp.float32), 0.1, 1.9),
        "w_query": draw_w_query(jax.random.fold_in(streams_of[9], 71), part),
        "w_latent": bell_draw(streams_of[4], (LAYERS, D, R), D ** -0.5, 0.125, ((0, 2),)),
        "latent_gain": jnp.clip(1.0 + 0.18 * jax.random.normal(streams_of[5], (LAYERS, R), jnp.float32), 0.1, 1.9),
        "w_key": bell_draw(streams_of[6], (LAYERS, R, HEADS * HD), R ** -0.5, 0.25, ((0, 2), (2, 4))),
        "w_value": bell_draw(streams_of[7], (LAYERS, R, HEADS * HD), R ** -0.5, 0.25, ((0, 2), (2, 4))),
        "w_out": bell_draw(streams_of[8], (LAYERS, HEADS * HD, D), (HEADS * HD) ** -0.5, 0.125, ((0, 2), (1, 4))),
    }


def rms_scale(values, gain):
    values = values.astype(jnp.float32)
    mean_sq = lax.optimization_barrier(jnp.mean(values * values, axis=-1, keepdims=True))
    return values * lax.rsqrt(mean_sq + 1e-06) * gain

def reference(hidden, lengths, attn_gain, w_query, w_latent, latent_gain, w_key, w_value, w_out):
    groups, group_rows, width = hidden.shape
    heads = w_key.shape[2] // HD
    rank = w_latent.shape[2]
    position = jnp.arange(group_rows, dtype=jnp.int32)
    block_ids = jnp.arange(groups, dtype=jnp.int32)
    live = position[None, :] < lengths[:, None]
    scale = 1.0 / HD ** 0.5
    state = hidden.astype(jnp.float32)
    stored = []
    for layer in range(LAYERS):
        normed = rms_scale(state, attn_gain[layer]).astype(jnp.bfloat16)
        flat = normed.reshape(groups * group_rows, width)
        query = jnp.dot(flat, w_query[layer], preferred_element_type=jnp.float32).astype(jnp.bfloat16)
        query = query.reshape(groups, group_rows, heads, HD)
        raw = jnp.dot(flat, w_latent[layer], preferred_element_type=jnp.float32)
        latent_full = rms_scale(raw, latent_gain[layer]).reshape(groups, group_rows, rank)
        latent = latent_full.astype(jnp.bfloat16)
        key_map = w_key[layer].astype(jnp.float32).reshape(rank, heads, HD)
        value_map = w_value[layer].astype(jnp.float32).reshape(rank, heads, HD)
        latent_wide = lax.optimization_barrier(latent).astype(jnp.float32)
        pieces = []
        for group in range(groups):
            seen = group + 1
            absorbed = (jnp.einsum('qhd,rhd->hqr', query[group].astype(jnp.float32), key_map) * scale).astype(jnp.bfloat16)
            absorbed_wide = lax.optimization_barrier(absorbed).astype(jnp.float32)
            keys_seen = latent_wide[:seen]
            scores = jnp.einsum('hqr,ckr->hqck', absorbed_wide, keys_seen)
            ids = block_ids[:seen]
            past = (ids < group)[:, None] & live[:seen]
            same = (ids == group)[None, :, None] & (position[None, None, :] <= position[:, None, None])
            mask = past[None] | same
            scores = jnp.where(mask[None], scores, -1e+30)
            top = lax.optimization_barrier(jnp.max(scores, axis=(2, 3), keepdims=True))
            weights = jnp.where(mask[None], jnp.exp(scores - top), 0.0)
            total = lax.optimization_barrier(jnp.sum(weights, axis=(2, 3)))
            rounded = lax.optimization_barrier(weights.astype(jnp.bfloat16)).astype(jnp.float32)
            context = jnp.einsum('hqck,ckr->hqr', rounded, keys_seen) / total[:, :, None]
            context = lax.optimization_barrier(context.astype(jnp.bfloat16)).astype(jnp.float32)
            attn = jnp.einsum('hqr,rhd->qhd', context, value_map)
            pieces.append(attn.reshape(group_rows, heads * HD).astype(jnp.bfloat16))
        attn_all = jnp.concatenate(pieces, axis=0)
        update = jnp.dot(attn_all, w_out[layer], preferred_element_type=jnp.float32)
        state = state + update.reshape(groups, group_rows, width)
        stored.append(jnp.where(live[:, :, None], latent_full, jnp.zeros_like(latent_full)))
    final = jnp.where(live[:, :, None], state, jnp.zeros_like(state))
    return (final, jnp.stack(stored, axis=0))
```

```python
import functools

import jax
import jax.numpy as jnp
from jax import lax
from jax.experimental import pallas as pl
from jax.experimental.pallas import tpu as pltpu
from jax.sharding import PartitionSpec as P

HD = 128
EPS = 1e-06
NEG = -1e30
FAR = 1 << 30
MESH = pl.DeviceIdType.MESH
LAST = (((1,), (1,)), ((), ()))


def rms_scale(values, gain):
    mean_sq = jnp.mean(values * values, axis=-1, keepdims=True)
    return values * lax.rsqrt(mean_sq + EPS) * gain


def dot(a, b):
    return jnp.dot(a, b, preferred_element_type=jnp.float32)


def dot_t(a, b):
    return lax.dot_general(a, b, LAST, preferred_element_type=jnp.float32)


def kernel(
    nz, nx, lengths, hid_hbm, gain, wq_hbm, wl_hbm, lgain, wk_hbm, wv_hbm, wo_hbm,
    final, lat, hid, wq, wl, wk, wv, wo, normed, kv, absorbed, top, total, accum, attn,
    part, headsum, xkeep, xhalf, finsum, load_sem, r_send, r_recv, l_send, l_recv,
    rs_send, rs_recv, ag_send, ag_recv, half_send, half_recv, fin_send, fin_recv,
):
    z, x, sec = lax.axis_index("seq"), lax.axis_index("head"), lax.axis_index("section")
    other = 1 - sec
    right, left = lax.rem(z + 1, nz), lax.rem(z + nz - 1, nz)
    groups, rows, width = hid.shape
    rank = wl.shape[1]
    heads = wk.shape[1] // HD
    share = rows // nx
    mine = groups * share
    half = width // 2
    mid = nz // 2
    hrows = heads * rows

    loads = [
        pltpu.make_async_copy(src, dst, load_sem.at[i])
        for i, (src, dst) in enumerate(
            [(hid_hbm, hid), (wl_hbm.at[0], wl), (wq_hbm.at[0], wq), (wk_hbm.at[0], wk), (wv_hbm.at[0], wv), (wo_hbm.at[0], wo)]
        )
    ]
    for load in loads:
        load.start()

    barrier = pltpu.get_barrier_semaphore()
    peers = [{"seq": right}, {"seq": left}]
    peers += [{"head": lax.rem(x + k, nx)} for k in range(1, nx)]
    peers += [{"section": other, "head": lax.rem(x + k, nx)} for k in range(nx)]
    for peer in peers:
        pl.semaphore_signal(barrier, inc=1, device_id=peer, device_id_type=MESH)
    pl.semaphore_wait(barrier, len(peers))

    def scatter_copy(h, owner, source):
        return pltpu.make_async_remote_copy(
            src_ref=part.at[h, owner], dst_ref=headsum.at[h, source],
            send_sem=rs_send.at[h, owner], recv_sem=rs_recv.at[h, source],
            device_id={"section": other, "head": owner}, device_id_type=MESH,
        )

    def normed_copy(to, source):
        return pltpu.make_async_remote_copy(
            src_ref=normed.at[source], dst_ref=normed.at[source],
            send_sem=ag_send.at[to], recv_sem=ag_recv.at[source],
            device_id={"head": to}, device_id_type=MESH,
        )

    def half_copy():
        return pltpu.make_async_remote_copy(
            src_ref=xkeep.at[0], dst_ref=xhalf, send_sem=half_send, recv_sem=half_recv,
            device_id={"section": other}, device_id_type=MESH,
        )

    loads[0].wait()

    @pl.when(sec == 0)
    def _():
        for b in range(groups):
            n = rms_scale(hid[b].astype(jnp.float32), gain[...]).astype(jnp.bfloat16)
            for o in range(nx):
                normed[o, b * share:(b + 1) * share] = n[o * share:(o + 1) * share]

    @pl.when(sec == 1)
    def _():
        for h in range(2):
            for s in range(nx):
                scatter_copy(h, s, s).wait_recv()
        for b in range(groups):
            at = pl.ds(b * share, share)
            own = hid[b, pl.ds(pl.multiple_of(x * share, share), share)].astype(jnp.float32)
            halves = []
            for h in range(2):
                summed = own[:, h * half:(h + 1) * half]
                add = headsum[h, 0, at].astype(jnp.float32)
                for s in range(1, nx):
                    add = add + headsum[h, s, at].astype(jnp.float32)
                halves.append(summed + add)
                xkeep[h, at] = halves[h]
            n = rms_scale(jnp.concatenate(halves, axis=1), gain[...])
            normed[x, at] = n.astype(jnp.bfloat16)
        for k in range(1, nx):
            normed_copy(lax.rem(x + k, nx), x).start()
        half_copy().start()
        for k in range(1, nx):
            normed_copy(x, lax.rem(x + k, nx)).wait_recv()

    def by_block(values, store):
        for o in range(nx):
            for b in range(groups):
                store(b, o, values[(o * groups + b) * share:(o * groups + b + 1) * share])

    flat = normed[...].reshape(nx * mine, width)
    loads[1].wait()
    latent_full = rms_scale(dot(flat, wl[...]), lgain[...])

    def store_latent(b, o, v):
        lat[0, b, o * share:(o + 1) * share] = v
        kv[z, b * rows + o * share:b * rows + (o + 1) * share] = v.astype(jnp.bfloat16)

    by_block(latent_full, store_latent)

    def ring_copy(tile, chunk, step, to, send, recv):
        at = pl.ds(chunk * rows, rows)
        return pltpu.make_async_remote_copy(
            src_ref=kv.at[tile, at], dst_ref=kv.at[tile, at],
            send_sem=send.at[step, chunk], recv_sem=recv.at[step, chunk],
            device_id={"seq": to}, device_id_type=MESH,
        )

    def to_right(tile, chunk, step):
        return ring_copy(tile, chunk, step, right, r_send, r_recv)

    def to_left(tile, chunk, step):
        return ring_copy(tile, chunk, step, left, l_send, l_recv)

    far_right = groups - groups // 2

    for c in range(groups):
        to_right(z, c, 0).start()
        to_left(z, c, 0).start()

    loads[2].wait()
    loads[3].wait()
    query = dot(normed[...].reshape(nx * mine, width), wq[...]).astype(jnp.bfloat16)
    for h in range(heads):
        cols = slice(h * HD, (h + 1) * HD)
        a = (dot_t(query[:, cols], wk[:, cols]) * (1.0 / HD**0.5)).astype(jnp.bfloat16)

        def store_absorbed(b, o, v):
            absorbed[b, h * rows + o * share:h * rows + (o + 1) * share] = v

        by_block(a, store_absorbed)

    def attend(tiles, first):
        for qb in range(groups):
            n = (qb + 1) * rows
            q = absorbed[qb]
            keys = jnp.concatenate([kv[t, :n] for t in tiles], axis=0) if len(tiles) > 1 else kv[tiles[0], :n]
            lane = lax.broadcasted_iota(jnp.int32, (1, n * len(tiles)), 1)
            at = lane % n
            tile = jnp.full_like(lane, tiles[0])
            for i, t in enumerate(tiles[1:]):
                tile = jnp.where(lane >= (i + 1) * n, t, tile)
            pos = tile * rows + at % rows
            limit = jnp.full_like(lane, lengths[0])
            for b in range(1, qb):
                limit = jnp.where(at >= b * rows, lengths[b], limit)
            key_at = jnp.where(at >= qb * rows, pos, jnp.where(pos < limit, -1, FAR))
            row_at = z * rows + lax.broadcasted_iota(jnp.int32, (hrows, 1), 0) % rows
            scores = jnp.where(key_at <= row_at, dot_t(q, keys), NEG)
            peak = jnp.max(scores, axis=1, keepdims=True)
            if first:
                weights = jnp.exp(scores - peak)
                total[qb] = jnp.sum(weights, axis=1, keepdims=True)
                accum[qb] = dot(weights.astype(jnp.bfloat16), keys)
                top[qb] = peak
            else:
                old = top[qb]
                peak = jnp.maximum(old, peak)
                shrink = jnp.exp(old - peak)
                weights = jnp.exp(scores - peak)
                total[qb] = total[qb] * shrink + jnp.sum(weights, axis=1, keepdims=True)
                accum[qb] = accum[qb] * shrink + dot(weights.astype(jnp.bfloat16), keys)
                top[qb] = peak

    attend([z], True)

    def ring_step(step, carry):
        from_left = lax.rem(z - step + nz, nz)
        from_right = lax.rem(z + step, nz)
        for c in range(groups):
            to_right(from_left, c, step - 1).wait_recv()

            @pl.when(jnp.logical_or(step < mid - 1, c < far_right))
            def _():
                to_right(from_left, c, step).start()

            to_left(from_right, c, step - 1).wait_recv()

            @pl.when(jnp.logical_or(step < mid - 1, c >= far_right))
            def _():
                to_left(from_right, c, step).start()

        attend([from_left, from_right], False)
        return carry

    lax.fori_loop(1, mid, ring_step, 0)
    last = lax.rem(z + mid, nz)
    for c in range(groups):
        (to_right if c < far_right else to_left)(last, c, mid - 1).wait_recv()
    attend([last], False)

    loads[4].wait()
    loads[5].wait()
    for h in range(heads):
        at = slice(h * rows, (h + 1) * rows)
        context = jnp.concatenate(
            [(accum[b, at] / total[b, at]).astype(jnp.bfloat16) for b in range(groups)], axis=0
        )
        cols = slice(h * HD, (h + 1) * HD)
        attn[:, cols] = dot(context, wv[:, cols]).astype(jnp.bfloat16)

    def finish_copy(h, owner, source):
        return pltpu.make_async_remote_copy(
            src_ref=part.at[h, owner], dst_ref=finsum.at[source],
            send_sem=fin_send.at[h, owner], recv_sem=fin_recv.at[source],
            device_id={"section": h, "head": owner}, device_id_type=MESH,
        )

    for h in range(2):
        out = dot(attn[...], wo[:, h * half:(h + 1) * half]).astype(jnp.bfloat16)
        for b in range(groups):
            for o in range(nx):
                part[h, o, b * share:(b + 1) * share] = out[b * rows + o * share:b * rows + (o + 1) * share]

        @pl.when(sec == 0)
        def _():
            for k in range(nx):
                scatter_copy(h, lax.rem(x + nx - 1 - k, nx), x).start()

        @pl.when(sec == 1)
        def _():
            for k in range(1 if h == 1 else 0, nx):
                finish_copy(h, lax.rem(x + k, nx), x).start()

    @pl.when(sec == 0)
    def _():
        half_copy().wait_recv()
        for s in range(nx):
            finish_copy(0, x, s).wait_recv()

    @pl.when(sec == 1)
    def _():
        finsum[x] = part[1, x]
        xhalf[...] = xkeep[1]
        for k in range(1, nx):
            finish_copy(1, x, lax.rem(x + k, nx)).wait_recv()

    for b in range(groups):
        at = pl.ds(b * share, share)
        add = finsum[0, at].astype(jnp.float32)
        for s in range(1, nx):
            add = add + finsum[s, at].astype(jnp.float32)
        final[b] = xhalf[at] + add

    @pl.when(sec == 0)
    def _():
        for h in range(2):
            for o in range(nx):
                scatter_copy(h, o, x).wait_send()

    @pl.when(sec == 1)
    def _():
        half_copy().wait_send()
        for k in range(1, nx):
            normed_copy(lax.rem(x + k, nx), x).wait_send()
        for h in range(2):
            for k in range(1 if h == 1 else 0, nx):
                finish_copy(h, lax.rem(x + k, nx), x).wait_send()

    def drain(step, carry):
        for c in range(groups):

            @pl.when(jnp.logical_or(step < mid - 1, c < far_right))
            def _():
                to_right(z, c, step).wait_send()

            @pl.when(jnp.logical_or(step < mid - 1, c >= far_right))
            def _():
                to_left(z, c, step).wait_send()

        return carry

    lax.fori_loop(0, mid, drain, 0)


def shards(nz, nx, hidden, lengths, attn_gain, w_query, w_latent, latent_gain, w_key, w_value, w_out):
    groups, rows, width = hidden.shape
    rank = w_latent.shape[2]
    cols = w_key.shape[2]
    heads = cols // HD
    share = rows // nx
    mine = groups * share
    half = width // 2
    mid = nz // 2
    vmem, dma = pltpu.VMEM, pltpu.SemaphoreType.DMA
    whole = pl.BlockSpec(memory_space=pltpu.VMEM)
    hbm = pl.BlockSpec(memory_space=pl.ANY)
    bf16, f32 = jnp.bfloat16, jnp.float32
    final, lat = pl.pallas_call(
        functools.partial(kernel, nz, nx),
        out_shape=(
            jax.ShapeDtypeStruct((groups, share, half), f32),
            jax.ShapeDtypeStruct((1, groups, rows, rank), f32),
        ),
        in_specs=[pl.BlockSpec(memory_space=pltpu.SMEM), hbm, whole, hbm, hbm, whole, hbm, hbm, hbm],
        out_specs=(whole, whole),
        scratch_shapes=[
            vmem((groups, rows, width), bf16),
            vmem((width, cols), bf16),
            vmem((width, rank), bf16),
            vmem((rank, cols), bf16),
            vmem((rank, cols), bf16),
            vmem((cols, width), bf16),
            vmem((nx, mine, width), bf16),
            vmem((nz, groups * rows, rank), bf16),
            vmem((groups, heads * rows, rank), bf16),
            vmem((groups, heads * rows, 1), f32),
            vmem((groups, heads * rows, 1), f32),
            vmem((groups, heads * rows, rank), f32),
            vmem((groups * rows, cols), bf16),
            vmem((2, nx, mine, half), bf16),
            vmem((2, nx, mine, half), bf16),
            vmem((2, mine, half), f32),
            vmem((mine, half), f32),
            vmem((nx, mine, half), bf16),
            dma((6,)),
            dma((mid, groups)),
            dma((mid, groups)),
            dma((mid, groups)),
            dma((mid, groups)),
            dma((2, nx)),
            dma((2, nx)),
            dma((nx,)),
            dma((nx,)),
            dma,
            dma,
            dma((2, nx)),
            dma((nx,)),
        ],
        compiler_params=pltpu.CompilerParams(
            collective_id=0, has_side_effects=True, vmem_limit_bytes=48 * 1024 * 1024
        ),
    )(lengths, hidden, attn_gain, w_query, w_latent, latent_gain, w_key, w_value, w_out)
    seq_id, head_id = lax.axis_index("seq"), lax.axis_index("head")
    pos = seq_id * rows + jnp.arange(rows, dtype=jnp.int32)
    live = pos[None, :] < lengths[:, None]
    out_pos = seq_id * rows + head_id * share + jnp.arange(share, dtype=jnp.int32)
    live_out = out_pos[None, :] < lengths[:, None]
    final = jnp.where(live_out[:, :, None], final, 0.0)
    lat = jnp.where(live[None, :, :, None], lat, 0.0)
    return (final, lat)


def solution(mesh):
    return jax.shard_map(
        functools.partial(shards, mesh.shape["seq"], mesh.shape["head"]),
        mesh=mesh,
        in_specs=(
            P("rep", "seq", None),
            P("rep"),
            P("section", None),
            P("section", None, "head"),
            P("section", None, None),
            P("section", None),
            P("section", None, "head"),
            P("section", None, "head"),
            P("section", "head", None),
        ),
        out_specs=(P("rep", ("seq", "head"), "section"), P("section", "rep", "seq", None)),
        check_vma=False,
    )
```

```python
import functools

import jax
import jax.numpy as jnp
from jax import lax
from jax.experimental import pallas as pl
from jax.experimental.pallas import tpu as pltpu
from jax.sharding import PartitionSpec as P

HD = 128
EPS = 1e-06
NEG = -1e30
MESH = pl.DeviceIdType.MESH
LAST = (((1,), (1,)), ((), ()))


def rms_scale(values, gain):
    mean_sq = jnp.mean(values * values, axis=-1, keepdims=True)
    return values * lax.rsqrt(mean_sq + EPS) * gain


def dot(a, b):
    return jnp.dot(a, b, preferred_element_type=jnp.float32)


def dot_t(a, b):
    return lax.dot_general(a, b, LAST, preferred_element_type=jnp.float32)


def kernel(
    nz, nx, len_hbm, hid_hbm, gain_hbm, wq_hbm, wl_hbm, lgain_hbm, wk_hbm, wv_hbm, wo_hbm,
    final, lat, lengths, hid, gain, lgain, wq, wl, wk, wv, wo, normed, kv, ownlat, absorbed, turned,
    top, total, accum, attn, part, headsum, xkeep, xhalf, finsum, load_sem,
    r_send, r_recv, l_send, l_recv, xa_send, xa_recv, xb_send, xb_recv, seed_send, seed_recv,
    rs_send, rs_recv, ag_send, ag_recv, half_send, half_recv, fin_send, fin_recv,
):
    z, x, sec = lax.axis_index("seq"), lax.axis_index("head"), lax.axis_index("section")
    other = 1 - sec
    x_up, x_down = lax.rem(x + 1, nx), lax.rem(x + nx - 1, nx)
    groups, rows, width = hid.shape
    rank = wl.shape[1]
    heads = wk.shape[1] // HD
    share = rows // nx
    mine = groups * share
    half = width // 2
    mid = nz // 2
    levels = mid // 2
    hrows = heads * rows

    loads = [
        pltpu.make_async_copy(src, dst, load_sem.at[i])
        for i, (src, dst) in enumerate(
            [
                (hid_hbm, hid), (gain_hbm, gain), (wl_hbm.at[0], wl), (lgain_hbm, lgain), (len_hbm, lengths),
                (wq_hbm.at[0], wq), (wk_hbm.at[0], wk), (wv_hbm.at[0], wv), (wo_hbm.at[0], wo),
            ]
        )
    ]
    for load in loads:
        load.start()

    barrier = pltpu.get_barrier_semaphore()
    peers = [{"seq": lax.rem(z + k, nz)} for k in (1, 2, nz - 2, nz - 1)]
    peers += [{"head": lax.rem(x + k, nx)} for k in range(1, nx)]
    peers += [{"section": other, "head": lax.rem(x + k, nx)} for k in range(nx)]
    for peer in peers:
        pl.semaphore_signal(barrier, inc=1, device_id=peer, device_id_type=MESH)

    def remote(src, dst, send, recv, to):
        return pltpu.make_async_remote_copy(
            src_ref=src, dst_ref=dst, send_sem=send, recv_sem=recv, device_id=to, device_id_type=MESH
        )

    def scatter_copy(h, owner, source):
        return remote(
            part.at[h, owner], headsum.at[h, source], rs_send.at[h, owner], rs_recv.at[h, source],
            {"section": other, "head": owner},
        )

    def normed_copy(to, source):
        return remote(normed.at[source], normed.at[source], ag_send.at[to], ag_recv.at[source], {"head": to})

    def half_copy():
        return remote(xkeep.at[0], xhalf, half_send, half_recv, {"section": other})

    def seed_copy(quarter):
        return remote(kv.at[z, quarter], kv.at[z, quarter], seed_send, seed_recv, {"head": x_down})

    def right_copy(d, hop, q):
        spot = kv.at[lax.rem(z + nz + hop - d, nz), lax.rem(x + q, nx)]
        return remote(spot, spot, r_send.at[d - 1, q], r_recv.at[d - 1, q], {"seq": lax.rem(z + hop, nz)})

    def left_copy(d, hop, q):
        spot = kv.at[lax.rem(z + nz - hop + d, nz), lax.rem(x + q, nx)]
        return remote(spot, spot, l_send.at[d - 1, q], l_recv.at[d - 1, q], {"seq": lax.rem(z + nz - hop, nz)})

    def up_copy(tile, slot, quarter):
        spot = kv.at[tile, quarter]
        return remote(spot, spot, xa_send.at[slot], xa_recv.at[slot], {"head": x_up})

    def down_copy(tile, slot, quarter):
        spot = kv.at[tile, quarter]
        return remote(spot, spot, xb_send.at[slot], xb_recv.at[slot], {"head": x_down})

    def across(tile, slot, q):
        if q == 0:
            up_copy(tile, slot, x).start()
        else:
            down_copy(tile, slot, x_up).start()

    def await_across(tile, slot):
        up_copy(tile, slot, x_down).wait_recv()
        down_copy(tile, slot, lax.rem(x + 2, nx)).wait_recv()

    def pieces(values):
        for o in range(nx):
            for b in range(groups):
                yield b, o, values[(o * groups + b) * share:(o * groups + b + 1) * share]

    def latents():
        flat = normed[...].reshape(nx * mine, width)
        full = rms_scale(dot(flat, wl[...]), lgain[...])
        for b, o, v in pieces(full):
            pos = z * rows + o * share + lax.broadcasted_iota(jnp.int32, (share, 1), 0)
            lat[0, b, o * share:(o + 1) * share] = jnp.where(pos < lengths[b], v, 0.0)
        return full.astype(jnp.bfloat16).reshape(nx, mine, rank)

    loads[0].wait()
    loads[1].wait()

    @pl.when(sec == 0)
    def _():
        for b in range(groups):
            n = rms_scale(hid[b].astype(jnp.float32), gain[...]).astype(jnp.bfloat16)
            for o in range(nx):
                normed[o, b * share:(b + 1) * share] = n[o * share:(o + 1) * share]

    for load in loads[2:5]:
        load.wait()

    @pl.when(sec == 0)
    def _():
        kv[z] = latents()

    with jax.named_scope("barrier"):
        pl.semaphore_wait(barrier, len(peers))

    @pl.when(sec == 1)
    def _():
        with jax.named_scope("rswait"):
            for h in range(2):
                for s in range(nx):
                    scatter_copy(h, s, s).wait_recv()
        for b in range(groups):
            at = pl.ds(b * share, share)
            own = hid[b, pl.ds(pl.multiple_of(x * share, share), share)].astype(jnp.float32)
            halves = []
            for h in range(2):
                add = headsum[h, 0, at].astype(jnp.float32)
                for s in range(1, nx):
                    add = add + headsum[h, s, at].astype(jnp.float32)
                halves.append(own[:, h * half:(h + 1) * half] + add)
                xkeep[h, at] = halves[h]
            n = rms_scale(jnp.concatenate(halves, axis=1), gain[...])
            normed[x, at] = n.astype(jnp.bfloat16)
        early = rms_scale(dot(normed[x], wl[...]), lgain[...])
        kv[z, x] = early.astype(jnp.bfloat16)
        seed_copy(x).start()

    def first_sends(q):
        for hop in (1, 2):
            right_copy(hop, hop, q).start()
            left_copy(hop, hop, q).start()

    first_sends(0)

    @pl.when(sec == 1)
    def _():
        for k in range(1, nx):
            normed_copy(lax.rem(x + k, nx), x).start()
        half_copy().start()
        with jax.named_scope("seedwait"):
            seed_copy(x_up).wait_recv()

    first_sends(1)

    @pl.when(sec == 1)
    def _():
        with jax.named_scope("agwait"):
            for k in range(1, nx):
                normed_copy(x, lax.rem(x + k, nx)).wait_recv()
        ownlat[...] = latents()
        for k in range(2, nx):
            o = lax.rem(x + k, nx)
            kv[z, o] = ownlat[o]

    loads[5].wait()
    loads[6].wait()
    with jax.named_scope("query"):
        query = dot(normed[...].reshape(nx * mine, width), wq[...]).astype(jnp.bfloat16)
        for h in range(heads):
            cols = slice(h * HD, (h + 1) * HD)
            a = (dot_t(query[:, cols], wk[:, cols]) * (1.0 / HD**0.5)).astype(jnp.bfloat16)
            for b, o, v in pieces(a):
                absorbed[b, h * rows + o * share:h * rows + (o + 1) * share] = v
        for b in range(groups):
            turned[b] = absorbed[b].T

    key_at = lax.broadcasted_iota(jnp.int32, (rows, hrows), 0)
    row_at = lax.broadcasted_iota(jnp.int32, (rows, hrows), 1) % rows

    def attend(tiles, own):
        keys, keep = [], {}
        for b in range(groups):
            for t in tiles:
                keys.append(kv[t, :, b * share:(b + 1) * share].reshape(rows, rank))
        keys = jnp.concatenate(keys, axis=0)
        keys_t = keys.T
        each = rows * len(tiles)

        def scores_of(qb):
            return dot(keys[:(qb + 1) * each], turned[qb])

        def fold(qb, scores):
            parts = []
            for b in range(qb + 1):
                for i, t in enumerate(tiles):
                    start = b * each + i * rows
                    s = scores[start:start + rows]
                    if b < qb:
                        seen = key_at < lengths[b] - t * rows
                    elif own:
                        seen = key_at <= row_at
                    else:
                        seen = key_at < jnp.where(t < z, rows, 0)
                    parts.append(jnp.where(seen, s, NEG))
            scores = jnp.concatenate(parts, axis=0)
            peak = jnp.max(scores, axis=0, keepdims=True)
            if not own:
                old = top[qb]
                peak = jnp.maximum(old, peak)
                shrink = jnp.exp(old - peak)
            weights = jnp.exp(scores - peak)
            add = jnp.sum(weights, axis=0, keepdims=True)
            gained = dot(keys_t[:, :(qb + 1) * each], weights.astype(jnp.bfloat16))
            if own:
                total[qb] = add
                accum[qb] = gained
            else:
                total[qb] = total[qb] * shrink + add
                accum[qb] = accum[qb] * shrink + gained
            top[qb] = peak

        ahead = scores_of(0)
        for qb in range(groups):
            now = ahead
            if qb + 1 < groups:
                ahead = scores_of(qb + 1)
            fold(qb, now)

    with jax.named_scope("attend_own"):
        attend([z], True)

    def tile_left(d):
        return lax.rem(z + nz - d, nz)

    def tile_right(d):
        return lax.rem(z + d, nz)

    def level(k, carry):
        near, deep = 2 * k + 1, 2 * k + 2

        @pl.when(k < levels)
        def _():
            with jax.named_scope("zwait"):
                for q in range(2):
                    right_copy(deep, 0, q).wait_recv()

                    @pl.when(k < levels - 1)
                    def _():
                        right_copy(deep + 1, 1, q).start()
                        right_copy(deep + 2, 2, q).start()

                    across(tile_left(deep), deep - 1, q)

                    @pl.when(k < levels - 1)
                    def _():
                        left_copy(deep, 0, q).wait_recv()
                        left_copy(deep + 1, 1, q).start()

                        @pl.when(k < levels - 2)
                        def _():
                            left_copy(deep + 2, 2, q).start()

                        across(tile_right(deep), mid + deep - 1, q)

                for q in range(2):
                    right_copy(near, 0, q).wait_recv()
                    across(tile_left(near), near - 1, q)
                    left_copy(near, 0, q).wait_recv()
                    across(tile_right(near), mid + near - 1, q)

        def pair(d, c):
            with jax.named_scope("xwait"):
                await_across(tile_left(d), d - 1)
                await_across(tile_right(d), mid + d - 1)
            with jax.named_scope("attend_pair"):
                attend([tile_left(d), tile_right(d)], False)
            return c

        lax.fori_loop(jnp.maximum(1, 2 * k - 1), jnp.minimum(2 * k, mid - 1) + 1, pair, 0)
        return carry

    lax.fori_loop(0, levels + 1, level, 0)
    with jax.named_scope("farwait"):
        await_across(tile_left(mid), mid - 1)
    with jax.named_scope("attend_far"):
        attend([tile_left(mid)], False)

    loads[7].wait()
    loads[8].wait()
    with jax.named_scope("value"):
        context = [(accum[b] / total[b]).astype(jnp.bfloat16).T for b in range(groups)]
        for h in range(heads):
            rows_h = jnp.concatenate([c[h * rows:(h + 1) * rows] for c in context], axis=0)
            cols = slice(h * HD, (h + 1) * HD)
            attn[:, cols] = dot(rows_h, wv[:, cols]).astype(jnp.bfloat16)

    def finish_copy(h, owner, source):
        return remote(
            part.at[h, owner], finsum.at[source], fin_send.at[h, owner], fin_recv.at[source],
            {"section": h, "head": owner},
        )

    for h in range(2):
        out = dot(attn[...], wo[:, h * half:(h + 1) * half]).astype(jnp.bfloat16)
        for b in range(groups):
            for o in range(nx):
                part[h, o, b * share:(b + 1) * share] = out[b * rows + o * share:b * rows + (o + 1) * share]

        @pl.when(sec == 0)
        def _():
            for k in range(nx):
                scatter_copy(h, lax.rem(x + nx - 1 - k, nx), x).start()

        @pl.when(sec == 1)
        def _():
            for k in range(1 if h == 1 else 0, nx):
                finish_copy(h, lax.rem(x + k, nx), x).start()

    @pl.when(sec == 0)
    def _():
        with jax.named_scope("finwait0"):
            half_copy().wait_recv()
            for s in range(nx):
                finish_copy(0, x, s).wait_recv()

    @pl.when(sec == 1)
    def _():
        finsum[x] = part[1, x]
        xhalf[...] = xkeep[1]
        with jax.named_scope("finwait1"):
            for k in range(1, nx):
                finish_copy(1, x, lax.rem(x + k, nx)).wait_recv()

    for b in range(groups):
        at = pl.ds(b * share, share)
        add = finsum[0, at].astype(jnp.float32)
        for s in range(1, nx):
            add = add + finsum[s, at].astype(jnp.float32)
        pos = z * rows + x * share + lax.broadcasted_iota(jnp.int32, (share, 1), 0)
        final[b] = jnp.where(pos < lengths[b], xhalf[at] + add, 0.0)

    @pl.when(sec == 0)
    def _():
        for h in range(2):
            for o in range(nx):
                scatter_copy(h, o, x).wait_send()

    @pl.when(sec == 1)
    def _():
        half_copy().wait_send()
        seed_copy(x).wait_send()
        for k in range(1, nx):
            normed_copy(lax.rem(x + k, nx), x).wait_send()
        for h in range(2):
            for k in range(1 if h == 1 else 0, nx):
                finish_copy(h, lax.rem(x + k, nx), x).wait_send()

    def drain(d, carry):
        for q in range(2):
            right_copy(d, 1, q).wait_send()

        up_copy(z, d - 1, x).wait_send()
        down_copy(z, d - 1, x).wait_send()

        @pl.when(d < mid)
        def _():
            for q in range(2):
                left_copy(d, 1, q).wait_send()

            up_copy(z, mid + d - 1, x).wait_send()
            down_copy(z, mid + d - 1, x).wait_send()

        return carry

    with jax.named_scope("drain"):
        lax.fori_loop(1, mid + 1, drain, 0)


def shards(nz, nx, hidden, lengths, attn_gain, w_query, w_latent, latent_gain, w_key, w_value, w_out):
    groups, rows, width = hidden.shape
    rank = w_latent.shape[2]
    cols = w_key.shape[2]
    heads = cols // HD
    share = rows // nx
    mine = groups * share
    half = width // 2
    mid = nz // 2
    vmem, dma = pltpu.VMEM, pltpu.SemaphoreType.DMA
    whole = pl.BlockSpec(memory_space=pltpu.VMEM)
    hbm = pl.BlockSpec(memory_space=pl.ANY)
    bf16, f32 = jnp.bfloat16, jnp.float32
    return pl.pallas_call(
        functools.partial(kernel, nz, nx),
        out_shape=(
            jax.ShapeDtypeStruct((groups, share, half), f32),
            jax.ShapeDtypeStruct((1, groups, rows, rank), f32),
        ),
        in_specs=[hbm] * 9,
        out_specs=(whole, whole),
        scratch_shapes=[
            pltpu.SMEM((groups,), jnp.int32),
            vmem((groups, rows, width), bf16),
            vmem((1, width), f32),
            vmem((1, rank), f32),
            vmem((width, cols), bf16),
            vmem((width, rank), bf16),
            vmem((rank, cols), bf16),
            vmem((rank, cols), bf16),
            vmem((cols, width), bf16),
            vmem((nx, mine, width), bf16),
            vmem((nz, nx, mine, rank), bf16),
            vmem((nx, mine, rank), bf16),
            vmem((groups, heads * rows, rank), bf16),
            vmem((groups, rank, heads * rows), bf16),
            vmem((groups, 1, heads * rows), f32),
            vmem((groups, 1, heads * rows), f32),
            vmem((groups, rank, heads * rows), f32),
            vmem((groups * rows, cols), bf16),
            vmem((2, nx, mine, half), bf16),
            vmem((2, nx, mine, half), bf16),
            vmem((2, mine, half), f32),
            vmem((mine, half), f32),
            vmem((nx, mine, half), bf16),
            dma((9,)),
            dma((mid, 2)),
            dma((mid, 2)),
            dma((mid, 2)),
            dma((mid, 2)),
            dma((nz - 1,)),
            dma((nz - 1,)),
            dma((nz - 1,)),
            dma((nz - 1,)),
            dma,
            dma,
            dma((2, nx)),
            dma((2, nx)),
            dma((nx,)),
            dma((nx,)),
            dma,
            dma,
            dma((2, nx)),
            dma((nx,)),
        ],
        compiler_params=pltpu.CompilerParams(
            collective_id=0, has_side_effects=True, vmem_limit_bytes=67043328
        ),
    )(lengths, hidden, attn_gain, w_query, w_latent, latent_gain, w_key, w_value, w_out)


def solution(mesh):
    return jax.shard_map(
        functools.partial(shards, mesh.shape["seq"], mesh.shape["head"]),
        mesh=mesh,
        in_specs=(
            P("rep", "seq", None),
            P("rep"),
            P("section", None),
            P("section", None, "head"),
            P("section", None, None),
            P("section", None),
            P("section", None, "head"),
            P("section", None, "head"),
            P("section", "head", None),
        ),
        out_specs=(P("rep", ("seq", "head"), "section"), P("section", "rep", "seq", None)),
        check_vma=False,
    )
```

```python
import functools

import jax
import jax.numpy as jnp
from jax import lax
from jax.experimental import pallas as pl
from jax.experimental.pallas import tpu as pltpu
from jax.sharding import PartitionSpec as P

HD = 128
EPS = 1e-06
NEG = -1e30
MESH = pl.DeviceIdType.MESH
LAST = (((1,), (1,)), ((), ()))


def rms_scale(values, gain):
    mean_sq = jnp.mean(values * values, axis=-1, keepdims=True)
    return values * lax.rsqrt(mean_sq + EPS) * gain


def dot(a, b):
    return jnp.dot(a, b, preferred_element_type=jnp.float32)


def dot_t(a, b):
    return lax.dot_general(a, b, LAST, preferred_element_type=jnp.float32)


def kernel(
    nz, nx, len_hbm, hid_hbm, gain_hbm, wq_hbm, wl_hbm, lgain_hbm, wk_hbm, wv_hbm, wo_hbm,
    final, lat, lengths, hid, gain, lgain, wq, wl, wk, wv, wo, normed, kv, ownlat, absorbed, turned, last_keys, last_turned,
    top, total, accum, attn, part, headsum, xkeep, xhalf, finsum, load_sem,
    r_send, r_recv, l_send, l_recv, xa_send, xa_recv, xb_send, xb_recv, seed_send, seed_recv,
    rs_send, rs_recv, ag_send, ag_recv, half_send, half_recv, fin_send, fin_recv,
):
    z, x, sec = lax.axis_index("seq"), lax.axis_index("head"), lax.axis_index("section")
    other = 1 - sec
    x_up, x_down = lax.rem(x + 1, nx), lax.rem(x + nx - 1, nx)
    groups, rows, width = hid.shape
    rank = wl.shape[1]
    heads = wk.shape[1] // HD
    share = rows // nx
    mine = groups * share
    half = width // 2
    mid = nz // 2
    levels = mid // 2
    hrows = heads * rows

    loads = [
        pltpu.make_async_copy(src, dst, load_sem.at[i])
        for i, (src, dst) in enumerate(
            [
                (hid_hbm, hid), (gain_hbm, gain), (wl_hbm.at[0], wl), (lgain_hbm, lgain), (len_hbm, lengths),
                (wq_hbm.at[0], wq), (wk_hbm.at[0], wk), (wv_hbm.at[0], wv), (wo_hbm.at[0], wo),
            ]
        )
    ]
    for load in loads:
        load.start()

    main = mine - share
    for o in range(nx):
        kv[:, o, main:] = jnp.zeros((nz, share, rank), kv.dtype)

    barrier = pltpu.get_barrier_semaphore()
    peers = [{"seq": lax.rem(z + k, nz)} for k in (1, 2, nz - 2, nz - 1)]
    peers += [{"head": lax.rem(x + k, nx)} for k in range(1, nx)]
    peers += [{"section": other, "head": lax.rem(x + k, nx)} for k in range(nx)]
    for peer in peers:
        pl.semaphore_signal(barrier, inc=1, device_id=peer, device_id_type=MESH)

    def remote(src, dst, send, recv, to):
        return pltpu.make_async_remote_copy(
            src_ref=src, dst_ref=dst, send_sem=send, recv_sem=recv, device_id=to, device_id_type=MESH
        )

    def scatter_copy(b, owner, source):
        return remote(
            part.at[b, owner], headsum.at[source, b], rs_send.at[b, owner], rs_recv.at[b, source],
            {"section": other, "head": owner},
        )

    def normed_copy(to, source):
        return remote(normed.at[source], normed.at[source], ag_send.at[to], ag_recv.at[source], {"head": to})

    def half_copy():
        return remote(xkeep.at[0], xhalf, half_send, half_recv, {"section": other})

    def seed_copy(quarter):
        return remote(kv.at[z, quarter], kv.at[z, quarter], seed_send, seed_recv, {"head": x_down})

    def tile_left(d):
        return lax.rem(z + nz - d, nz)

    def tile_right(d):
        return lax.rem(z + d, nz)

    def either(carry, make, act):
        @pl.when(carry)
        def _():
            getattr(make(mine), act)()

        @pl.when(jnp.logical_not(carry))
        def _():
            getattr(make(main), act)()

    def right_copy(d, hop, q, act):
        tile = tile_left(d - hop)

        def make(count):
            spot = kv.at[tile, lax.rem(x + q, nx), pl.ds(0, count)]
            return remote(spot, spot, r_send.at[d - 1, q], r_recv.at[d - 1, q], {"seq": tile_right(hop)})

        either(tile + d < nz, make, act)

    def left_copy(d, hop, q, deep, act):
        tile = tile_right(d - hop)

        def make(count):
            spot = kv.at[tile, lax.rem(x + q, nx), pl.ds(0, count)]
            return remote(spot, spot, l_send.at[d - 1, q], l_recv.at[d - 1, q], {"seq": tile_left(hop)})

        either(tile < mid - 1 if deep else tile < d, make, act)

    def up_copy(tile, slot, quarter, act):
        def make(count):
            spot = kv.at[tile, quarter, pl.ds(0, count)]
            return remote(spot, spot, xa_send.at[slot], xa_recv.at[slot], {"head": x_up})

        either(tile <= z, make, act)

    def down_copy(tile, slot, quarter, act):
        def make(count):
            spot = kv.at[tile, quarter, pl.ds(0, count)]
            return remote(spot, spot, xb_send.at[slot], xb_recv.at[slot], {"head": x_down})

        either(tile <= z, make, act)

    def across(tile, slot, q):
        if q == 0:
            up_copy(tile, slot, x, "start")
        else:
            down_copy(tile, slot, x_up, "start")

    def await_across(tile, slot):
        up_copy(tile, slot, x_down, "wait_recv")
        down_copy(tile, slot, lax.rem(x + 2, nx), "wait_recv")

    def pieces(values):
        for o in range(nx):
            for b in range(groups):
                yield b, o, values[(o * groups + b) * share:(o * groups + b + 1) * share]

    def latents():
        flat = normed[...].reshape(nx * mine, width)
        full = rms_scale(dot(flat, wl[...]), lgain[...])
        for b, o, v in pieces(full):
            pos = z * rows + o * share + lax.broadcasted_iota(jnp.int32, (share, 1), 0)
            lat[0, b, o * share:(o + 1) * share] = jnp.where(pos < lengths[b], v, 0.0)
        return full.astype(jnp.bfloat16).reshape(nx, mine, rank)

    loads[0].wait()
    loads[1].wait()

    @pl.when(sec == 0)
    def _():
        for b in range(groups):
            n = rms_scale(hid[b].astype(jnp.float32), gain[...]).astype(jnp.bfloat16)
            for o in range(nx):
                normed[o, b * share:(b + 1) * share] = n[o * share:(o + 1) * share]

    for load in loads[2:5]:
        load.wait()

    @pl.when(sec == 0)
    def _():
        kv[z] = latents()

    with jax.named_scope("barrier"):
        pl.semaphore_wait(barrier, len(peers))

    @pl.when(sec == 1)
    def _():
        for b in range(groups):
            with jax.named_scope("rswait"):
                for k in range(nx):
                    scatter_copy(b, x, k).wait_recv()
            at = pl.ds(b * share, share)
            own = hid[b, pl.ds(pl.multiple_of(x * share, share), share)].astype(jnp.float32)
            halves = []
            for h in range(2):
                add = headsum[0, b, h].astype(jnp.float32)
                for k in range(1, nx):
                    add = add + headsum[k, b, h].astype(jnp.float32)
                halves.append(own[:, h * half:(h + 1) * half] + add)
                xkeep[h, at] = halves[h]
            n = rms_scale(jnp.concatenate(halves, axis=1), gain[...])
            normed[x, at] = n.astype(jnp.bfloat16)
        early = rms_scale(dot(normed[x], wl[...]), lgain[...])
        kv[z, x] = early.astype(jnp.bfloat16)
        seed_copy(x).start()

    def first_sends(q):
        for hop in (2, 1):
            right_copy(hop, hop, q, "start")
            left_copy(hop, hop, q, hop == 2, "start")

    first_sends(0)

    @pl.when(sec == 1)
    def _():
        for k in range(1, nx):
            normed_copy(lax.rem(x + k, nx), x).start()
        half_copy().start()
        with jax.named_scope("seedwait"):
            seed_copy(x_up).wait_recv()

    first_sends(1)

    def arrive(k):
        near, deep = 2 * k + 1, 2 * k + 2
        with jax.named_scope("zwait"):
            for q in range(2):
                right_copy(deep, 0, q, "wait_recv")

                @pl.when(k < levels - 1)
                def _():
                    right_copy(deep + 2, 2, q, "start")
                    left_copy(deep, 0, q, True, "wait_recv")

                @pl.when(k < levels - 2)
                def _():
                    left_copy(deep + 2, 2, q, True, "start")

            for q in range(2):

                @pl.when(k < levels - 1)
                def _():
                    right_copy(deep + 1, 1, q, "start")
                    left_copy(deep + 1, 1, q, False, "start")
                    across(tile_right(deep), mid + deep - 1, q)

                across(tile_left(deep), deep - 1, q)
            for q in range(2):
                right_copy(near, 0, q, "wait_recv")
                across(tile_left(near), near - 1, q)
                left_copy(near, 0, q, False, "wait_recv")
                across(tile_right(near), mid + near - 1, q)

    arrive(0)

    @pl.when(sec == 1)
    def _():
        with jax.named_scope("agwait"):
            for k in range(1, nx):
                normed_copy(x, lax.rem(x + k, nx)).wait_recv()
        ownlat[...] = latents()
        for k in range(2, nx):
            o = lax.rem(x + k, nx)
            kv[z, o] = ownlat[o]

    loads[5].wait()
    loads[6].wait()
    with jax.named_scope("query"):
        query = dot(normed[...].reshape(nx * mine, width), wq[...]).astype(jnp.bfloat16)
        for h in range(heads):
            cols = slice(h * HD, (h + 1) * HD)
            a = (dot_t(query[:, cols], wk[:, cols]) * (1.0 / HD**0.5)).astype(jnp.bfloat16)
            for b, o, v in pieces(a):
                absorbed[b, h * rows + o * share:h * rows + (o + 1) * share] = v
        for b in range(groups):
            turned[b] = absorbed[b].T

    key_at = lax.broadcasted_iota(jnp.int32, (rows, hrows), 0)
    row_at = lax.broadcasted_iota(jnp.int32, (rows, hrows), 1) % rows

    def gather_keys(tiles):
        keys = []
        for b in range(groups):
            for t in tiles:
                keys.append(kv[t, :, b * share:(b + 1) * share].reshape(rows, rank))
        keys = jnp.concatenate(keys, axis=0)
        return keys, keys.T

    def fold(qb, scores, keys_t, tiles, own, light):
        parts = []
        each = rows * len(tiles)
        blocks = qb if light else qb + 1
        for b in range(blocks):
            for i, t in enumerate(tiles):
                start = b * each + i * rows
                s = scores[start:start + rows]
                if b < qb:
                    seen = key_at < lengths[b] - t * rows
                elif own:
                    seen = key_at <= row_at
                else:
                    seen = key_at < jnp.where(t < z, rows, 0)
                parts.append(jnp.where(seen, s, NEG))
        scores = jnp.concatenate(parts, axis=0)
        peak = jnp.max(scores, axis=0, keepdims=True)
        if not own:
            old = top[qb]
            peak = jnp.maximum(old, peak)
            shrink = jnp.exp(old - peak)
        weights = jnp.exp(scores - peak)
        add = jnp.sum(weights, axis=0, keepdims=True)
        gained = dot(keys_t, weights.astype(jnp.bfloat16))
        if own:
            total[qb] = add
            accum[qb] = gained
        else:
            total[qb] = total[qb] * shrink + add
            accum[qb] = accum[qb] * shrink + gained
        top[qb] = peak

    def attend(tiles, own, light):
        keys, keys_t = gather_keys(tiles)
        each = rows * len(tiles)

        def count(qb):
            return (qb if light else qb + 1) * each

        start = 1 if light else 0
        ahead = dot(keys[:count(start)], turned[start])
        for qb in range(start, groups):
            now = ahead
            if qb + 1 < groups:
                ahead = dot(keys[:count(qb + 1)], turned[qb + 1])
            fold(qb, now, keys_t[:, :count(qb)], tiles, own, light)

    with jax.named_scope("attend_own"):
        attend([z], True, False)

    def level(k, carry):
        arrive(k)

        def pair(d, c):
            with jax.named_scope("xwait"):
                await_across(tile_left(d), d - 1)
                await_across(tile_right(d), mid + d - 1)
            light = jnp.logical_and(z < d, z + d < nz)

            @pl.when(light)
            def _():
                with jax.named_scope("attend_light"):
                    attend([tile_left(d), tile_right(d)], False, True)

            @pl.when(jnp.logical_not(light))
            def _():
                with jax.named_scope("attend_pair"):
                    attend([tile_left(d), tile_right(d)], False, False)

            return c

        lax.fori_loop(2 * k - 1, 2 * k + 1, pair, 0)
        return carry

    lax.fori_loop(1, levels, level, 0)
    ends = [tile_left(mid - 1), tile_right(mid - 1), tile_left(mid)]
    with jax.named_scope("farwait"):
        await_across(ends[0], mid - 2)
        await_across(ends[1], 2 * mid - 2)
        await_across(ends[2], mid - 1)
    end_keys, end_turned = gather_keys(ends)
    last_keys[...] = end_keys
    last_turned[...] = end_turned
    all_later = z < mid - 1

    for load in loads[7:]:
        load.wait()

    def finish_copy(b, h, owner, source):
        return remote(
            part.at[b, owner, h], finsum.at[source, b], fin_send.at[b, h, owner], fin_recv.at[b, source],
            {"section": h, "head": owner},
        )

    for b in range(groups):

        def last_fold(light):
            n = (b if light else b + 1) * len(ends) * rows
            fold(b, dot(last_keys[:n], turned[b]), last_turned[:, :n], ends, False, light)

        with jax.named_scope("attend_last"):
            if b > 0:

                @pl.when(all_later)
                def _():
                    last_fold(True)

            @pl.when(jnp.logical_not(all_later))
            def _():
                last_fold(False)

        with jax.named_scope("project"):
            context = (accum[b] / total[b]).astype(jnp.bfloat16).T
            for h in range(heads):
                cols = slice(h * HD, (h + 1) * HD)
                attn[:, cols] = dot(context[h * rows:(h + 1) * rows], wv[:, cols]).astype(jnp.bfloat16)
            for h in range(2):
                out = dot(attn[...], wo[:, h * half:(h + 1) * half]).astype(jnp.bfloat16)
                for o in range(nx):
                    part[b, o, h] = out[o * share:(o + 1) * share]

        @pl.when(sec == 0)
        def _():
            for k in range(nx):
                scatter_copy(b, lax.rem(x + nx - 1 - k, nx), x).start()

        @pl.when(sec == 1)
        def _():
            for k in range(1, nx):
                for h in range(2):
                    finish_copy(b, h, lax.rem(x + k, nx), x).start()
            finish_copy(b, 0, x, x).start()

    @pl.when(sec == 0)
    def _():
        half_copy().wait_recv()

    @pl.when(sec == 1)
    def _():
        xhalf[...] = xkeep[1]

    for b in range(groups):

        @pl.when(sec == 0)
        def _():
            with jax.named_scope("finwait0"):
                for k in range(nx):
                    finish_copy(b, 0, x, k).wait_recv()

        @pl.when(sec == 1)
        def _():
            finsum[x, b] = part[b, x, 1]
            with jax.named_scope("finwait1"):
                for k in range(1, nx):
                    finish_copy(b, 1, x, lax.rem(x + k, nx)).wait_recv()

        at = pl.ds(b * share, share)
        add = finsum[0, b].astype(jnp.float32)
        for k in range(1, nx):
            add = add + finsum[k, b].astype(jnp.float32)
        pos = z * rows + x * share + lax.broadcasted_iota(jnp.int32, (share, 1), 0)
        final[b] = jnp.where(pos < lengths[b], xhalf[at] + add, 0.0)

    @pl.when(sec == 0)
    def _():
        for b in range(groups):
            for o in range(nx):
                scatter_copy(b, o, x).wait_send()

    @pl.when(sec == 1)
    def _():
        half_copy().wait_send()
        seed_copy(x).wait_send()
        for k in range(1, nx):
            normed_copy(lax.rem(x + k, nx), x).wait_send()
        for b in range(groups):
            for k in range(1, nx):
                for h in range(2):
                    finish_copy(b, h, lax.rem(x + k, nx), x).wait_send()
            finish_copy(b, 0, x, x).wait_send()

    def drain(k, carry):
        for d, hop in ((2 * k + 1, 1), (2 * k + 2, 2)):
            for q in range(2):
                right_copy(d, hop, q, "wait_send")
            up_copy(tile_left(d), d - 1, x, "wait_send")
            down_copy(tile_left(d), d - 1, x, "wait_send")

            @pl.when(d < mid)
            def _():
                for q in range(2):
                    left_copy(d, hop, q, hop == 2, "wait_send")
                up_copy(tile_right(d), mid + d - 1, x, "wait_send")
                down_copy(tile_right(d), mid + d - 1, x, "wait_send")

        return carry

    with jax.named_scope("drain"):
        lax.fori_loop(0, levels, drain, 0)


def shards(nz, nx, hidden, lengths, attn_gain, w_query, w_latent, latent_gain, w_key, w_value, w_out):
    groups, rows, width = hidden.shape
    rank = w_latent.shape[2]
    cols = w_key.shape[2]
    heads = cols // HD
    share = rows // nx
    mine = groups * share
    half = width // 2
    mid = nz // 2
    vmem, dma = pltpu.VMEM, pltpu.SemaphoreType.DMA
    whole = pl.BlockSpec(memory_space=pltpu.VMEM)
    hbm = pl.BlockSpec(memory_space=pl.ANY)
    bf16, f32 = jnp.bfloat16, jnp.float32
    return pl.pallas_call(
        functools.partial(kernel, nz, nx),
        out_shape=(
            jax.ShapeDtypeStruct((groups, share, half), f32),
            jax.ShapeDtypeStruct((1, groups, rows, rank), f32),
        ),
        in_specs=[hbm] * 9,
        out_specs=(whole, whole),
        scratch_shapes=[
            pltpu.SMEM((groups,), jnp.int32),
            vmem((groups, rows, width), bf16),
            vmem((1, width), f32),
            vmem((1, rank), f32),
            vmem((width, cols), bf16),
            vmem((width, rank), bf16),
            vmem((rank, cols), bf16),
            vmem((rank, cols), bf16),
            vmem((cols, width), bf16),
            vmem((nx, mine, width), bf16),
            vmem((nz, nx, mine, rank), bf16),
            vmem((nx, mine, rank), bf16),
            vmem((groups, heads * rows, rank), bf16),
            vmem((groups, rank, heads * rows), bf16),
            vmem((3 * groups * rows, rank), bf16),
            vmem((rank, 3 * groups * rows), bf16),
            vmem((groups, 1, heads * rows), f32),
            vmem((groups, 1, heads * rows), f32),
            vmem((groups, rank, heads * rows), f32),
            vmem((rows, cols), bf16),
            vmem((groups, nx, 2, share, half), bf16),
            vmem((nx, groups, 2, share, half), bf16),
            vmem((2, mine, half), f32),
            vmem((mine, half), f32),
            vmem((nx, groups, share, half), bf16),
            dma((9,)),
            dma((mid, 2)),
            dma((mid, 2)),
            dma((mid, 2)),
            dma((mid, 2)),
            dma((nz - 1,)),
            dma((nz - 1,)),
            dma((nz - 1,)),
            dma((nz - 1,)),
            dma,
            dma,
            dma((groups, nx)),
            dma((groups, nx)),
            dma((nx,)),
            dma((nx,)),
            dma,
            dma,
            dma((groups, 2, nx)),
            dma((groups, nx)),
        ],
        compiler_params=pltpu.CompilerParams(
            collective_id=0, has_side_effects=True, vmem_limit_bytes=67043328
        ),
    )(lengths, hidden, attn_gain, w_query, w_latent, latent_gain, w_key, w_value, w_out)


def solution(mesh):
    return jax.shard_map(
        functools.partial(shards, mesh.shape["seq"], mesh.shape["head"]),
        mesh=mesh,
        in_specs=(
            P("rep", "seq", None),
            P("rep"),
            P("section", None),
            P("section", None, "head"),
            P("section", None, None),
            P("section", None),
            P("section", None, "head"),
            P("section", None, "head"),
            P("section", "head", None),
        ),
        out_specs=(P("rep", ("seq", "head"), "section"), P("section", "rep", "seq", None)),
        check_vma=False,
    )
```

```python
import functools

import jax
import jax.numpy as jnp
from jax import lax
from jax.experimental import pallas as pl
from jax.experimental.pallas import tpu as pltpu
from jax.sharding import PartitionSpec as P

HD = 128
EPS = 1e-06
NEG = -1e30
MESH = pl.DeviceIdType.MESH
LAST = (((1,), (1,)), ((), ()))


def rms_scale(values, gain):
    mean_sq = jnp.mean(values * values, axis=-1, keepdims=True)
    return values * lax.rsqrt(mean_sq + EPS) * gain


def dot(a, b):
    return jnp.dot(a, b, preferred_element_type=jnp.float32)


def dot_t(a, b):
    return lax.dot_general(a, b, LAST, preferred_element_type=jnp.float32)


def kernel(
    nz, nx, small, hid_hbm, wq_hbm, wl_hbm, wk_hbm, wv_hbm, wo_hbm,
    final, lat, counts, hid, wq, wl, wk, wv, wo, normed, kv, ownlat, absorbed, turned, last_keys, last_turned,
    top, total, accum, attn, part, headsum, xkeep, xhalf, finsum, load_sem,
    r_send, r_recv, l_send, l_recv, xa_send, xa_recv, xb_send, xb_recv, seed_send, seed_recv,
    rs_send, rs_recv, ag_send, ag_recv, half_send, half_recv, fin_send, fin_recv,
):
    z, x, sec = lax.axis_index("seq"), lax.axis_index("head"), lax.axis_index("section")
    other = 1 - sec
    x_up, x_down = lax.rem(x + 1, nx), lax.rem(x + nx - 1, nx)
    groups, rows, width = hid.shape
    rank = wl.shape[1]
    heads = wk.shape[1] // HD
    share = rows // nx
    mine = groups * share
    half = width // 2
    mid = nz // 2
    levels = mid // 2
    hrows = heads * rows

    loads = [
        pltpu.make_async_copy(src, dst, load_sem.at[i])
        for i, (src, dst) in enumerate(
            [
                (hid_hbm, hid), (small.at[:, width + rank:], counts), (wl_hbm.at[0], wl),
                (wq_hbm.at[0], wq), (wk_hbm.at[0], wk), (wv_hbm.at[0], wv), (wo_hbm.at[0], wo),
            ]
        )
    ]
    for load in loads:
        load.start()

    main = mine - share
    for o in range(nx):
        kv[:, o, main:] = jnp.zeros((nz, share, rank), kv.dtype)

    barrier = pltpu.get_barrier_semaphore()
    peers = [{"seq": lax.rem(z + k, nz)} for k in (1, 2, nz - 2, nz - 1)]
    peers += [{"head": lax.rem(x + k, nx)} for k in range(1, nx)]
    peers += [{"section": other, "head": lax.rem(x + k, nx)} for k in range(nx)]
    for peer in peers:
        pl.semaphore_signal(barrier, inc=1, device_id=peer, device_id_type=MESH)

    def remote(src, dst, send, recv, to):
        return pltpu.make_async_remote_copy(
            src_ref=src, dst_ref=dst, send_sem=send, recv_sem=recv, device_id=to, device_id_type=MESH
        )

    def scatter_copy(b, owner, source):
        return remote(
            part.at[b, owner], headsum.at[source, b], rs_send.at[b, owner], rs_recv.at[b, source],
            {"section": other, "head": owner},
        )

    def normed_copy(to, source):
        return remote(normed.at[source], normed.at[source], ag_send.at[to], ag_recv.at[source], {"head": to})

    def half_copy():
        return remote(xkeep.at[0], xhalf, half_send, half_recv, {"section": other})

    def seed_copy(quarter):
        return remote(kv.at[z, quarter], kv.at[z, quarter], seed_send, seed_recv, {"head": x_down})

    def tile_left(d):
        return lax.rem(z + nz - d, nz)

    def tile_right(d):
        return lax.rem(z + d, nz)

    def either(carry, make, act):
        @pl.when(carry)
        def _():
            getattr(make(mine), act)()

        @pl.when(jnp.logical_not(carry))
        def _():
            getattr(make(main), act)()

    def right_copy(d, hop, q, act):
        tile = tile_left(d - hop)

        def make(count):
            spot = kv.at[tile, lax.rem(x + q, nx), pl.ds(0, count)]
            return remote(spot, spot, r_send.at[d - 1, q], r_recv.at[d - 1, q], {"seq": tile_right(hop)})

        either(tile + d < nz, make, act)

    def left_copy(d, hop, q, deep, act):
        tile = tile_right(d - hop)

        def make(count):
            spot = kv.at[tile, lax.rem(x + q, nx), pl.ds(0, count)]
            return remote(spot, spot, l_send.at[d - 1, q], l_recv.at[d - 1, q], {"seq": tile_left(hop)})

        either(tile < mid - 1 if deep else tile < d, make, act)

    def up_copy(tile, slot, quarter, act):
        def make(count):
            spot = kv.at[tile, quarter, pl.ds(0, count)]
            return remote(spot, spot, xa_send.at[slot], xa_recv.at[slot], {"head": x_up})

        either(tile <= z, make, act)

    def down_copy(tile, slot, quarter, act):
        def make(count):
            spot = kv.at[tile, quarter, pl.ds(0, count)]
            return remote(spot, spot, xb_send.at[slot], xb_recv.at[slot], {"head": x_down})

        either(tile <= z, make, act)

    def across(tile, slot, q):
        if q == 0:
            up_copy(tile, slot, x, "start")
        else:
            down_copy(tile, slot, x_up, "start")

    def await_across(tile, slot):
        up_copy(tile, slot, x_down, "wait_recv")
        down_copy(tile, slot, lax.rem(x + 2, nx), "wait_recv")

    def pieces(values):
        for o in range(nx):
            for b in range(groups):
                yield b, o, values[(o * groups + b) * share:(o * groups + b + 1) * share]

    def latents():
        flat = normed[...].reshape(nx * mine, width)
        full = rms_scale(dot(flat, wl[...]), lgain)
        for b, o, v in pieces(full):
            pos = z * rows + o * share + lax.broadcasted_iota(jnp.int32, (share, 1), 0)
            lat[0, b, o * share:(o + 1) * share] = jnp.where(pos < lengths[b], v, 0.0)
        return full.astype(jnp.bfloat16).reshape(nx, mine, rank)

    gain, lgain = small[:, :width], small[:, width:width + rank]
    loads[0].wait()
    loads[1].wait()
    lengths = [counts[0, b].astype(jnp.int32) for b in range(groups)]

    @pl.when(sec == 0)
    def _():
        for b in range(groups):
            n = rms_scale(hid[b].astype(jnp.float32), gain).astype(jnp.bfloat16)
            for o in range(nx):
                normed[o, b * share:(b + 1) * share] = n[o * share:(o + 1) * share]

    loads[2].wait()

    @pl.when(sec == 0)
    def _():
        kv[z] = latents()

    with jax.named_scope("barrier"):
        pl.semaphore_wait(barrier, len(peers))

    @pl.when(sec == 1)
    def _():
        for b in range(groups):
            with jax.named_scope("rswait"):
                for k in range(nx):
                    scatter_copy(b, x, k).wait_recv()
            at = pl.ds(b * share, share)
            own = hid[b, pl.ds(pl.multiple_of(x * share, share), share)].astype(jnp.float32)
            halves = []
            for h in range(2):
                add = headsum[0, b, h].astype(jnp.float32)
                for k in range(1, nx):
                    add = add + headsum[k, b, h].astype(jnp.float32)
                halves.append(own[:, h * half:(h + 1) * half] + add)
                xkeep[h, at] = halves[h]
            n = rms_scale(jnp.concatenate(halves, axis=1), gain)
            normed[x, at] = n.astype(jnp.bfloat16)
        early = rms_scale(dot(normed[x], wl[...]), lgain)
        kv[z, x] = early.astype(jnp.bfloat16)
        seed_copy(x).start()

    def first_sends(q):
        for hop in (2, 1):
            right_copy(hop, hop, q, "start")
            left_copy(hop, hop, q, hop == 2, "start")

    first_sends(0)

    @pl.when(sec == 1)
    def _():
        for k in range(1, nx):
            normed_copy(lax.rem(x + k, nx), x).start()
        half_copy().start()
        with jax.named_scope("seedwait"):
            seed_copy(x_up).wait_recv()

    first_sends(1)

    def arrive(k):
        near, deep = 2 * k + 1, 2 * k + 2
        with jax.named_scope("zwait"):
            for q in range(2):
                right_copy(deep, 0, q, "wait_recv")

                @pl.when(k < levels - 1)
                def _():
                    right_copy(deep + 2, 2, q, "start")
                    left_copy(deep, 0, q, True, "wait_recv")

                @pl.when(k < levels - 2)
                def _():
                    left_copy(deep + 2, 2, q, True, "start")

            for q in range(2):

                @pl.when(k < levels - 1)
                def _():
                    right_copy(deep + 1, 1, q, "start")
                    left_copy(deep + 1, 1, q, False, "start")
                    across(tile_right(deep), mid + deep - 1, q)

                across(tile_left(deep), deep - 1, q)
            for q in range(2):
                right_copy(near, 0, q, "wait_recv")
                across(tile_left(near), near - 1, q)
                left_copy(near, 0, q, False, "wait_recv")
                across(tile_right(near), mid + near - 1, q)

    arrive(0)

    @pl.when(sec == 1)
    def _():
        with jax.named_scope("agwait"):
            for k in range(1, nx):
                normed_copy(x, lax.rem(x + k, nx)).wait_recv()

    loads[3].wait()
    loads[4].wait()
    with jax.named_scope("query"):
        query = dot(normed[...].reshape(nx * mine, width), wq[...]).astype(jnp.bfloat16)
        for h in range(heads):
            cols = slice(h * HD, (h + 1) * HD)
            a = (dot_t(query[:, cols], wk[:, cols]) * (1.0 / HD**0.5)).astype(jnp.bfloat16)
            for b, o, v in pieces(a):
                absorbed[b, h * rows + o * share:h * rows + (o + 1) * share] = v
        for b in range(groups):
            turned[b] = absorbed[b].T

    arrive(1)

    @pl.when(sec == 1)
    def _():
        with jax.named_scope("latents"):
            ownlat[...] = latents()
            for k in range(2, nx):
                o = lax.rem(x + k, nx)
                kv[z, o] = ownlat[o]

    key_at = lax.broadcasted_iota(jnp.int32, (rows, hrows), 0)
    row_at = lax.broadcasted_iota(jnp.int32, (rows, hrows), 1) % rows

    def gather_keys(tiles):
        keys = []
        for b in range(groups):
            for t in tiles:
                keys.append(kv[t, :, b * share:(b + 1) * share].reshape(rows, rank))
        keys = jnp.concatenate(keys, axis=0)
        return keys, keys.T

    def fold(qb, scores, keys_t, tiles, own, light):
        parts = []
        each = rows * len(tiles)
        blocks = qb if light else qb + 1
        for b in range(blocks):
            for i, t in enumerate(tiles):
                start = b * each + i * rows
                s = scores[start:start + rows]
                if b < qb:
                    seen = key_at < lengths[b] - t * rows
                elif own:
                    seen = key_at <= row_at
                else:
                    seen = key_at < jnp.where(t < z, rows, 0)
                parts.append(jnp.where(seen, s, NEG))
        scores = jnp.concatenate(parts, axis=0)
        peak = jnp.max(scores, axis=0, keepdims=True)
        if not own:
            old = top[qb]
            peak = jnp.maximum(old, peak)
            shrink = jnp.exp(old - peak)
        weights = jnp.exp(scores - peak)
        add = jnp.sum(weights, axis=0, keepdims=True)
        gained = dot(keys_t, weights.astype(jnp.bfloat16))
        if own:
            total[qb] = add
            accum[qb] = gained
        else:
            total[qb] = total[qb] * shrink + add
            accum[qb] = accum[qb] * shrink + gained
        top[qb] = peak

    def attend(tiles, own, light):
        keys, keys_t = gather_keys(tiles)
        each = rows * len(tiles)

        def count(qb):
            return (qb if light else qb + 1) * each

        start = 1 if light else 0
        ahead = dot(keys[:count(start)], turned[start])
        for qb in range(start, groups):
            now = ahead
            if qb + 1 < groups:
                ahead = dot(keys[:count(qb + 1)], turned[qb + 1])
            fold(qb, now, keys_t[:, :count(qb)], tiles, own, light)

    with jax.named_scope("attend_own"):
        attend([z], True, False)

    def level(k, carry):
        @pl.when(k > 1)
        def _():
            arrive(k)

        def pair(d, c):
            with jax.named_scope("xwait"):
                await_across(tile_left(d), d - 1)
                await_across(tile_right(d), mid + d - 1)
            light = jnp.logical_and(z < d, z + d < nz)

            @pl.when(light)
            def _():
                with jax.named_scope("attend_light"):
                    attend([tile_left(d), tile_right(d)], False, True)

            @pl.when(jnp.logical_not(light))
            def _():
                with jax.named_scope("attend_pair"):
                    attend([tile_left(d), tile_right(d)], False, False)

            return c

        lax.fori_loop(2 * k - 1, 2 * k + 1, pair, 0)
        return carry

    lax.fori_loop(1, levels, level, 0)
    ends = [tile_left(mid - 1), tile_right(mid - 1), tile_left(mid)]
    with jax.named_scope("farwait"):
        await_across(ends[0], mid - 2)
        await_across(ends[1], 2 * mid - 2)
        await_across(ends[2], mid - 1)
    end_keys, end_turned = gather_keys(ends)
    last_keys[...] = end_keys
    last_turned[...] = end_turned
    all_later = z < mid - 1

    for load in loads[5:]:
        load.wait()

    def finish_copy(b, h, owner, source):
        return remote(
            part.at[b, owner, h], finsum.at[source, b], fin_send.at[b, h, owner], fin_recv.at[b, source],
            {"section": h, "head": owner},
        )

    for b in range(groups):

        def last_fold(light):
            n = (b if light else b + 1) * len(ends) * rows
            fold(b, dot(last_keys[:n], turned[b]), last_turned[:, :n], ends, False, light)

        with jax.named_scope("attend_last"):
            if b > 0:

                @pl.when(all_later)
                def _():
                    last_fold(True)

            @pl.when(jnp.logical_not(all_later))
            def _():
                last_fold(False)

        with jax.named_scope("project"):
            context = (accum[b] / total[b]).astype(jnp.bfloat16).T
            for h in range(heads):
                cols = slice(h * HD, (h + 1) * HD)
                attn[:, cols] = dot(context[h * rows:(h + 1) * rows], wv[:, cols]).astype(jnp.bfloat16)
            for h in range(2):
                out = dot(attn[...], wo[:, h * half:(h + 1) * half]).astype(jnp.bfloat16)
                for o in range(nx):
                    part[b, o, h] = out[o * share:(o + 1) * share]

        @pl.when(sec == 0)
        def _():
            for k in range(nx):
                scatter_copy(b, lax.rem(x + nx - 1 - k, nx), x).start()

        @pl.when(sec == 1)
        def _():
            for k in range(1, nx):
                for h in range(2):
                    finish_copy(b, h, lax.rem(x + k, nx), x).start()
            finish_copy(b, 0, x, x).start()

    def drain(k, carry):
        for d, hop in ((2 * k + 1, 1), (2 * k + 2, 2)):
            for q in range(2):
                right_copy(d, hop, q, "wait_send")
            up_copy(tile_left(d), d - 1, x, "wait_send")
            down_copy(tile_left(d), d - 1, x, "wait_send")

            @pl.when(d < mid)
            def _():
                for q in range(2):
                    left_copy(d, hop, q, hop == 2, "wait_send")
                up_copy(tile_right(d), mid + d - 1, x, "wait_send")
                down_copy(tile_right(d), mid + d - 1, x, "wait_send")

        return carry

    with jax.named_scope("drain"):
        lax.fori_loop(0, levels, drain, 0)

    @pl.when(sec == 0)
    def _():
        half_copy().wait_recv()
        for b in range(groups):
            for o in range(nx):
                scatter_copy(b, o, x).wait_send()

    @pl.when(sec == 1)
    def _():
        xhalf[...] = xkeep[1]
        half_copy().wait_send()
        seed_copy(x).wait_send()
        for k in range(1, nx):
            normed_copy(lax.rem(x + k, nx), x).wait_send()

    for b in range(groups):

        @pl.when(sec == 0)
        def _():
            with jax.named_scope("finwait0"):
                for k in range(nx):
                    finish_copy(b, 0, x, k).wait_recv()

        @pl.when(sec == 1)
        def _():
            finsum[x, b] = part[b, x, 1]
            with jax.named_scope("finwait1"):
                for k in range(1, nx):
                    finish_copy(b, 1, x, lax.rem(x + k, nx)).wait_recv()

        at = pl.ds(b * share, share)
        add = finsum[0, b].astype(jnp.float32)
        for k in range(1, nx):
            add = add + finsum[k, b].astype(jnp.float32)
        pos = z * rows + x * share + lax.broadcasted_iota(jnp.int32, (share, 1), 0)
        final[b] = jnp.where(pos < lengths[b], xhalf[at] + add, 0.0)

    @pl.when(sec == 1)
    def _():
        for b in range(groups):
            for k in range(1, nx):
                for h in range(2):
                    finish_copy(b, h, lax.rem(x + k, nx), x).wait_send()
            finish_copy(b, 0, x, x).wait_send()


def shards(nz, nx, hidden, lengths, attn_gain, w_query, w_latent, latent_gain, w_key, w_value, w_out):
    groups, rows, width = hidden.shape
    rank = w_latent.shape[2]
    cols = w_key.shape[2]
    heads = cols // HD
    share = rows // nx
    mine = groups * share
    half = width // 2
    mid = nz // 2
    vmem, dma = pltpu.VMEM, pltpu.SemaphoreType.DMA
    whole = pl.BlockSpec(memory_space=pltpu.VMEM)
    hbm = pl.BlockSpec(memory_space=pl.ANY)
    counts = jnp.pad(lengths[None], ((0, 0), (0, 128 - groups))).astype(jnp.float32)
    small = jnp.concatenate([attn_gain, latent_gain, counts], axis=1)
    bf16, f32 = jnp.bfloat16, jnp.float32
    return pl.pallas_call(
        functools.partial(kernel, nz, nx),
        out_shape=(
            jax.ShapeDtypeStruct((groups, share, half), f32),
            jax.ShapeDtypeStruct((1, groups, rows, rank), f32),
        ),
        in_specs=[whole] + [hbm] * 6,
        out_specs=(whole, whole),
        scratch_shapes=[
            pltpu.SMEM((1, 128), f32),
            vmem((groups, rows, width), bf16),
            vmem((width, cols), bf16),
            vmem((width, rank), bf16),
            vmem((rank, cols), bf16),
            vmem((rank, cols), bf16),
            vmem((cols, width), bf16),
            vmem((nx, mine, width), bf16),
            vmem((nz, nx, mine, rank), bf16),
            vmem((nx, mine, rank), bf16),
            vmem((groups, heads * rows, rank), bf16),
            vmem((groups, rank, heads * rows), bf16),
            vmem((3 * groups * rows, rank), bf16),
            vmem((rank, 3 * groups * rows), bf16),
            vmem((groups, 1, heads * rows), f32),
            vmem((groups, 1, heads * rows), f32),
            vmem((groups, rank, heads * rows), f32),
            vmem((rows, cols), bf16),
            vmem((groups, nx, 2, share, half), bf16),
            vmem((nx, groups, 2, share, half), bf16),
            vmem((2, mine, half), f32),
            vmem((mine, half), f32),
            vmem((nx, groups, share, half), bf16),
            dma((7,)),
            dma((mid, 2)),
            dma((mid, 2)),
            dma((mid, 2)),
            dma((mid, 2)),
            dma((nz - 1,)),
            dma((nz - 1,)),
            dma((nz - 1,)),
            dma((nz - 1,)),
            dma,
            dma,
            dma((groups, nx)),
            dma((groups, nx)),
            dma((nx,)),
            dma((nx,)),
            dma,
            dma,
            dma((groups, 2, nx)),
            dma((groups, nx)),
        ],
        compiler_params=pltpu.CompilerParams(
            collective_id=0, has_side_effects=True, vmem_limit_bytes=54500 * 1024
        ),
    )(small, hidden, w_query, w_latent, w_key, w_value, w_out)


def solution(mesh):
    return jax.shard_map(
        functools.partial(shards, mesh.shape["seq"], mesh.shape["head"]),
        mesh=mesh,
        in_specs=(
            P("rep", "seq", None),
            P("rep"),
            P("section", None),
            P("section", None, "head"),
            P("section", None, None),
            P("section", None),
            P("section", None, "head"),
            P("section", None, "head"),
            P("section", "head", None),
        ),
        out_specs=(P("rep", ("seq", "head"), "section"), P("section", "rep", "seq", None)),
        check_vma=False,
    )
```

```python
import functools

import jax
import jax.numpy as jnp
from jax import lax
from jax.experimental import pallas as pl
from jax.experimental.pallas import tpu as pltpu
from jax.sharding import PartitionSpec as P

HD = 128
EPS = 1e-06
NEG = -1e30
MESH = pl.DeviceIdType.MESH
LAST = (((1,), (1,)), ((), ()))


def rms_scale(values, gain):
    mean_sq = jnp.mean(values * values, axis=-1, keepdims=True)
    return values * lax.rsqrt(mean_sq + EPS) * gain


def dot(a, b):
    return jnp.dot(a, b, preferred_element_type=jnp.float32)


def dot_t(a, b):
    return lax.dot_general(a, b, LAST, preferred_element_type=jnp.float32)


def kernel(
    nz, nx, small, hid_hbm, wq_hbm, wl_hbm, wk_hbm, wv_hbm, wo_hbm,
    final_out, lat_out, final, lat, out_sem, counts, hid, wq, wl, wk, wv, wo, normed, kv, ownlat, absorbed, turned, last_keys, last_turned,
    top, total, accum, attn, part, headsum, xkeep, xhalf, finsum, load_sem,
    r_send, r_recv, l_send, l_recv, xa_send, xa_recv, xb_send, xb_recv, seed_send, seed_recv,
    rs_send, rs_recv, ag_send, ag_recv, half_send, half_recv, fin_send, fin_recv,
):
    z, x, sec = lax.axis_index("seq"), lax.axis_index("head"), lax.axis_index("section")
    other = 1 - sec
    x_up, x_down = lax.rem(x + 1, nx), lax.rem(x + nx - 1, nx)
    groups, rows, width = hid.shape
    rank = wl.shape[1]
    heads = wk.shape[1] // HD
    share = rows // nx
    mine = groups * share
    half = width // 2
    mid = nz // 2
    levels = mid // 2
    hrows = heads * rows

    loads = [
        pltpu.make_async_copy(src, dst, load_sem.at[i])
        for i, (src, dst) in enumerate(
            [
                (hid_hbm, hid), (small.at[:, width + rank:], counts), (wl_hbm.at[0], wl),
                (wq_hbm.at[0], wq), (wk_hbm.at[0], wk), (wv_hbm.at[0], wv), (wo_hbm.at[0], wo),
            ]
        )
    ]
    for load in loads:
        load.start()

    main = mine - share
    for o in range(nx):
        kv[:, o, main:] = jnp.zeros((nz, share, rank), kv.dtype)

    barrier = pltpu.get_barrier_semaphore()
    peers = [{"seq": lax.rem(z + k, nz)} for k in (1, 2, nz - 2, nz - 1)]
    peers += [{"head": lax.rem(x + k, nx)} for k in range(1, nx)]
    peers += [{"section": other, "head": lax.rem(x + k, nx)} for k in range(nx)]
    for peer in peers:
        pl.semaphore_signal(barrier, inc=1, device_id=peer, device_id_type=MESH)

    def remote(src, dst, send, recv, to):
        return pltpu.make_async_remote_copy(
            src_ref=src, dst_ref=dst, send_sem=send, recv_sem=recv, device_id=to, device_id_type=MESH
        )

    def scatter_copy(b, h, owner, source):
        return remote(
            part.at[b, owner, h], headsum.at[source, b, h], rs_send.at[b, h, owner], rs_recv.at[b, h, source],
            {"section": other, "head": owner},
        )

    def normed_copy(to, source):
        return remote(normed.at[source], normed.at[source], ag_send.at[to], ag_recv.at[source], {"head": to})

    def half_copy():
        return remote(xkeep.at[0], xhalf, half_send, half_recv, {"section": other})

    def seed_copy(quarter):
        return remote(kv.at[z, quarter], kv.at[z, quarter], seed_send, seed_recv, {"head": x_down})

    def tile_left(d):
        return lax.rem(z + nz - d, nz)

    def tile_right(d):
        return lax.rem(z + d, nz)

    def either(carry, make, act):
        @pl.when(carry)
        def _():
            getattr(make(mine), act)()

        @pl.when(jnp.logical_not(carry))
        def _():
            getattr(make(main), act)()

    def right_copy(d, hop, q, act):
        tile = tile_left(d - hop)

        def make(count):
            spot = kv.at[tile, lax.rem(x + q, nx), pl.ds(0, count)]
            return remote(spot, spot, r_send.at[d - 1, q], r_recv.at[d - 1, q], {"seq": tile_right(hop)})

        either(tile + d < nz, make, act)

    def left_copy(d, hop, q, deep, act):
        tile = tile_right(d - hop)

        def make(count):
            spot = kv.at[tile, lax.rem(x + q, nx), pl.ds(0, count)]
            return remote(spot, spot, l_send.at[d - 1, q], l_recv.at[d - 1, q], {"seq": tile_left(hop)})

        either(tile < mid - 1 if deep else tile < d, make, act)

    def up_copy(tile, slot, quarter, act):
        def make(count):
            spot = kv.at[tile, quarter, pl.ds(0, count)]
            return remote(spot, spot, xa_send.at[slot], xa_recv.at[slot], {"head": x_up})

        either(tile <= z, make, act)

    def down_copy(tile, slot, quarter, act):
        def make(count):
            spot = kv.at[tile, quarter, pl.ds(0, count)]
            return remote(spot, spot, xb_send.at[slot], xb_recv.at[slot], {"head": x_down})

        either(tile <= z, make, act)

    def across(tile, slot, q):
        if q == 0:
            up_copy(tile, slot, x, "start")
        else:
            down_copy(tile, slot, x_up, "start")

    def await_across(tile, slot):
        up_copy(tile, slot, x_down, "wait_recv")
        down_copy(tile, slot, lax.rem(x + 2, nx), "wait_recv")

    def pieces(values):
        for o in range(nx):
            for b in range(groups):
                yield b, o, values[(o * groups + b) * share:(o * groups + b + 1) * share]

    lat_copy = pltpu.make_async_copy(lat, lat_out, out_sem.at[groups])

    def latents():
        flat = normed[...].reshape(nx * mine, width)
        full = rms_scale(dot(flat, wl[...]), lgain)
        for b, o, v in pieces(full):
            pos = z * rows + o * share + lax.broadcasted_iota(jnp.int32, (share, 1), 0)
            lat[0, b, o * share:(o + 1) * share] = jnp.where(pos < lengths[b], v, 0.0)
        lat_copy.start()
        return full.astype(jnp.bfloat16).reshape(nx, mine, rank)

    def normed_of(k):
        o = lax.rem(x + k, nx)
        at = pl.ds(pl.multiple_of(o * share, share), share)
        raw = jnp.concatenate([hid[b, at].astype(jnp.float32) for b in range(groups)], axis=0)
        normed[o] = rms_scale(raw, gain).astype(jnp.bfloat16)

    def fill_own():
        ownlat[...] = latents()
        for k in range(2, nx):
            o = lax.rem(x + k, nx)
            kv[z, o] = ownlat[o]

    gain, lgain = small[:, :width], small[:, width:width + rank]
    loads[0].wait()
    loads[1].wait()
    lengths = [counts[0, b].astype(jnp.int32) for b in range(groups)]

    @pl.when(sec == 0)
    def _():
        normed_of(0)
        normed_of(1)

    loads[2].wait()

    @pl.when(sec == 0)
    def _():
        rows_now = jnp.concatenate([normed[x], normed[x_up]], axis=0)
        early = rms_scale(dot(rows_now, wl[...]), lgain).astype(jnp.bfloat16)
        kv[z, x] = early[:mine]
        kv[z, x_up] = early[mine:]

    with jax.named_scope("barrier"):
        pl.semaphore_wait(barrier, len(peers))

    @pl.when(sec == 1)
    def _():
        for b in range(groups):
            with jax.named_scope("rswait"):
                for h in range(2):
                    for k in range(nx):
                        scatter_copy(b, h, x, k).wait_recv()
            at = pl.ds(b * share, share)
            own = hid[b, pl.ds(pl.multiple_of(x * share, share), share)].astype(jnp.float32)
            halves = []
            for h in range(2):
                add = headsum[0, b, h].astype(jnp.float32)
                for k in range(1, nx):
                    add = add + headsum[k, b, h].astype(jnp.float32)
                halves.append(own[:, h * half:(h + 1) * half] + add)
                xkeep[h, at] = halves[h]
            n = rms_scale(jnp.concatenate(halves, axis=1), gain)
            normed[x, at] = n.astype(jnp.bfloat16)
        early = rms_scale(dot(normed[x], wl[...]), lgain)
        kv[z, x] = early.astype(jnp.bfloat16)
        seed_copy(x).start()

    def first_sends(q):
        for hop in (2, 1):
            right_copy(hop, hop, q, "start")
            left_copy(hop, hop, q, hop == 2, "start")

    first_sends(0)

    @pl.when(sec == 1)
    def _():
        for k in range(1, nx):
            normed_copy(lax.rem(x + k, nx), x).start()
        half_copy().start()
        with jax.named_scope("seedwait"):
            seed_copy(x_up).wait_recv()

    first_sends(1)

    def arrive(k):
        near, deep = 2 * k + 1, 2 * k + 2
        with jax.named_scope("zwait"):
            for q in range(2):
                right_copy(deep, 0, q, "wait_recv")

                @pl.when(k < levels - 1)
                def _():
                    right_copy(deep + 2, 2, q, "start")
                    left_copy(deep, 0, q, True, "wait_recv")

                @pl.when(k < levels - 2)
                def _():
                    left_copy(deep + 2, 2, q, True, "start")

            for q in range(2):

                @pl.when(k < levels - 1)
                def _():
                    right_copy(deep + 1, 1, q, "start")
                    left_copy(deep + 1, 1, q, False, "start")
                    across(tile_right(deep), mid + deep - 1, q)

                across(tile_left(deep), deep - 1, q)
            for q in range(2):
                right_copy(near, 0, q, "wait_recv")
                across(tile_left(near), near - 1, q)
                left_copy(near, 0, q, False, "wait_recv")
                across(tile_right(near), mid + near - 1, q)

    @pl.when(sec == 0)
    def _():
        with jax.named_scope("fill"):
            for k in range(2, nx):
                normed_of(k)
            fill_own()

    arrive(0)

    @pl.when(sec == 1)
    def _():
        with jax.named_scope("agwait"):
            for k in range(1, nx):
                normed_copy(x, lax.rem(x + k, nx)).wait_recv()
        fill_own()

    loads[3].wait()
    loads[4].wait()
    with jax.named_scope("query"):
        query = dot(normed[...].reshape(nx * mine, width), wq[...]).astype(jnp.bfloat16)
        for h in range(heads):
            cols = slice(h * HD, (h + 1) * HD)
            a = (dot_t(query[:, cols], wk[:, cols]) * (1.0 / HD**0.5)).astype(jnp.bfloat16)
            for b, o, v in pieces(a):
                absorbed[b, h * rows + o * share:h * rows + (o + 1) * share] = v
        for b in range(groups):
            turned[b] = absorbed[b].T

    key_at = lax.broadcasted_iota(jnp.int32, (rows, hrows), 0)
    row_at = lax.broadcasted_iota(jnp.int32, (rows, hrows), 1) % rows

    def gather_keys(tiles):
        keys = []
        for b in range(groups):
            for t in tiles:
                keys.append(kv[t, :, b * share:(b + 1) * share].reshape(rows, rank))
        keys = jnp.concatenate(keys, axis=0)
        return keys, keys.T

    def fold(qb, scores, keys_t, tiles, own, light):
        parts = []
        each = rows * len(tiles)
        blocks = qb if light else qb + 1
        for b in range(blocks):
            for i, t in enumerate(tiles):
                start = b * each + i * rows
                s = scores[start:start + rows]
                if b < qb:
                    seen = key_at < lengths[b] - t * rows
                elif own:
                    seen = key_at <= row_at
                else:
                    seen = key_at < jnp.where(t < z, rows, 0)
                parts.append(jnp.where(seen, s, NEG))
        scores = jnp.concatenate(parts, axis=0)
        peak = jnp.max(scores, axis=0, keepdims=True)
        if not own:
            old = top[qb]
            peak = jnp.maximum(old, peak)
            shrink = jnp.exp(old - peak)
        weights = jnp.exp(scores - peak)
        add = jnp.sum(weights, axis=0, keepdims=True)
        gained = dot(keys_t, weights.astype(jnp.bfloat16))
        if own:
            total[qb] = add
            accum[qb] = gained
        else:
            total[qb] = total[qb] * shrink + add
            accum[qb] = accum[qb] * shrink + gained
        top[qb] = peak

    def attend(tiles, own, light):
        keys, keys_t = gather_keys(tiles)
        each = rows * len(tiles)

        def count(qb):
            return (qb if light else qb + 1) * each

        start = 1 if light else 0
        ahead = dot(keys[:count(start)], turned[start])
        for qb in range(start, groups):
            now = ahead
            if qb + 1 < groups:
                ahead = dot(keys[:count(qb + 1)], turned[qb + 1])
            fold(qb, now, keys_t[:, :count(qb)], tiles, own, light)

    with jax.named_scope("attend_own"):
        attend([z], True, False)

    def level(k, carry):
        arrive(k)

        def pair(d, c):
            with jax.named_scope("xwait"):
                await_across(tile_left(d), d - 1)
                await_across(tile_right(d), mid + d - 1)
            light = jnp.logical_and(z < d, z + d < nz)

            @pl.when(light)
            def _():
                with jax.named_scope("attend_light"):
                    attend([tile_left(d), tile_right(d)], False, True)

            @pl.when(jnp.logical_not(light))
            def _():
                with jax.named_scope("attend_pair"):
                    attend([tile_left(d), tile_right(d)], False, False)

            return c

        lax.fori_loop(2 * k - 1, 2 * k + 1, pair, 0)
        return carry

    lax.fori_loop(1, levels, level, 0)
    ends = [tile_left(mid - 1), tile_right(mid - 1), tile_left(mid)]
    with jax.named_scope("farwait"):
        await_across(ends[0], mid - 2)
        await_across(ends[1], 2 * mid - 2)
        await_across(ends[2], mid - 1)
    end_keys, end_turned = gather_keys(ends)
    last_keys[...] = end_keys
    last_turned[...] = end_turned
    all_later = z < mid - 1

    for load in loads[5:]:
        load.wait()

    def finish_copy(b, h, owner, source):
        return remote(
            part.at[b, owner, h], finsum.at[source, b], fin_send.at[b, h, owner], fin_recv.at[b, source],
            {"section": h, "head": owner},
        )

    for b in range(groups):

        def last_fold(light):
            n = (b if light else b + 1) * len(ends) * rows
            fold(b, dot(last_keys[:n], turned[b]), last_turned[:, :n], ends, False, light)

        with jax.named_scope("attend_last"):
            if b > 0:

                @pl.when(all_later)
                def _():
                    last_fold(True)

            @pl.when(jnp.logical_not(all_later))
            def _():
                last_fold(False)

        with jax.named_scope("project"):
            context = (accum[b] / total[b]).astype(jnp.bfloat16).T
            for h in range(heads):
                cols = slice(h * HD, (h + 1) * HD)
                attn[:, cols] = dot(context[h * rows:(h + 1) * rows], wv[:, cols]).astype(jnp.bfloat16)
        for h in range(2):
            with jax.named_scope("out"):
                out = dot(attn[...], wo[:, h * half:(h + 1) * half]).astype(jnp.bfloat16)
                for o in range(nx):
                    part[b, o, h] = out[o * share:(o + 1) * share]

            @pl.when(sec == 0)
            def _():
                for k in range(nx):
                    scatter_copy(b, h, lax.rem(x + nx - 1 - k, nx), x).start()

            @pl.when(sec == 1)
            def _():
                for k in range(1 if h == 1 else 0, nx):
                    finish_copy(b, h, lax.rem(x + k, nx), x).start()

    def drain(k, carry):
        for d, hop in ((2 * k + 1, 1), (2 * k + 2, 2)):
            for q in range(2):
                right_copy(d, hop, q, "wait_send")
            up_copy(tile_left(d), d - 1, x, "wait_send")
            down_copy(tile_left(d), d - 1, x, "wait_send")

            @pl.when(d < mid)
            def _():
                for q in range(2):
                    left_copy(d, hop, q, hop == 2, "wait_send")
                up_copy(tile_right(d), mid + d - 1, x, "wait_send")
                down_copy(tile_right(d), mid + d - 1, x, "wait_send")

        return carry

    with jax.named_scope("drain"):
        lax.fori_loop(0, levels, drain, 0)

    @pl.when(sec == 0)
    def _():
        half_copy().wait_recv()
        for b in range(groups):
            for h in range(2):
                for o in range(nx):
                    scatter_copy(b, h, o, x).wait_send()

    @pl.when(sec == 1)
    def _():
        xhalf[...] = xkeep[1]
        half_copy().wait_send()
        seed_copy(x).wait_send()
        for k in range(1, nx):
            normed_copy(lax.rem(x + k, nx), x).wait_send()

    for b in range(groups):

        @pl.when(sec == 0)
        def _():
            with jax.named_scope("finwait0"):
                for k in range(nx):
                    finish_copy(b, 0, x, k).wait_recv()

        @pl.when(sec == 1)
        def _():
            finsum[x, b] = part[b, x, 1]
            with jax.named_scope("finwait1"):
                for k in range(1, nx):
                    finish_copy(b, 1, x, lax.rem(x + k, nx)).wait_recv()

        at = pl.ds(b * share, share)
        add = finsum[0, b].astype(jnp.float32)
        for k in range(1, nx):
            add = add + finsum[k, b].astype(jnp.float32)
        pos = z * rows + x * share + lax.broadcasted_iota(jnp.int32, (share, 1), 0)
        final[b] = jnp.where(pos < lengths[b], xhalf[at] + add, 0.0)
        pltpu.make_async_copy(final.at[b], final_out.at[b], out_sem.at[b]).start()

    @pl.when(sec == 1)
    def _():
        for b in range(groups):
            for k in range(1, nx):
                for h in range(2):
                    finish_copy(b, h, lax.rem(x + k, nx), x).wait_send()
            finish_copy(b, 0, x, x).wait_send()

    lat_copy.wait()
    for b in range(groups):
        pltpu.make_async_copy(final.at[b], final_out.at[b], out_sem.at[b]).wait()


def shards(nz, nx, hidden, lengths, attn_gain, w_query, w_latent, latent_gain, w_key, w_value, w_out):
    groups, rows, width = hidden.shape
    rank = w_latent.shape[2]
    cols = w_key.shape[2]
    heads = cols // HD
    share = rows // nx
    mine = groups * share
    half = width // 2
    mid = nz // 2
    vmem, dma = pltpu.VMEM, pltpu.SemaphoreType.DMA
    whole = pl.BlockSpec(memory_space=pltpu.VMEM)
    hbm = pl.BlockSpec(memory_space=pl.ANY)
    bf16, f32 = jnp.bfloat16, jnp.float32
    flat = ((0, 0, 0),)
    pieces = (attn_gain, latent_gain, lengths[None])
    size, at, small = width + rank + 128, 0, 0.0
    for piece in pieces:
        count = piece.shape[1]
        zero = jnp.zeros((), piece.dtype)
        small = small + lax.pad(piece, zero, flat + ((at, size - at - count, 0),)).astype(f32)
        at += count
    return pl.pallas_call(
        functools.partial(kernel, nz, nx),
        out_shape=(
            jax.ShapeDtypeStruct((groups, share, half), f32),
            jax.ShapeDtypeStruct((1, groups, rows, rank), f32),
        ),
        in_specs=[whole] + [hbm] * 6,
        out_specs=(hbm, hbm),
        scratch_shapes=[
            vmem((groups, share, half), f32),
            vmem((1, groups, rows, rank), f32),
            dma((groups + 1,)),
            pltpu.SMEM((1, 128), f32),
            vmem((groups, rows, width), bf16),
            vmem((width, cols), bf16),
            vmem((width, rank), bf16),
            vmem((rank, cols), bf16),
            vmem((rank, cols), bf16),
            vmem((cols, width), bf16),
            vmem((nx, mine, width), bf16),
            vmem((nz, nx, mine, rank), bf16),
            vmem((nx, mine, rank), bf16),
            vmem((groups, heads * rows, rank), bf16),
            vmem((groups, rank, heads * rows), bf16),
            vmem((3 * groups * rows, rank), bf16),
            vmem((rank, 3 * groups * rows), bf16),
            vmem((groups, 1, heads * rows), f32),
            vmem((groups, 1, heads * rows), f32),
            vmem((groups, rank, heads * rows), f32),
            vmem((rows, cols), bf16),
            vmem((groups, nx, 2, share, half), bf16),
            vmem((nx, groups, 2, share, half), bf16),
            vmem((2, mine, half), f32),
            vmem((mine, half), f32),
            vmem((nx, groups, share, half), bf16),
            dma((7,)),
            dma((mid, 2)),
            dma((mid, 2)),
            dma((mid, 2)),
            dma((mid, 2)),
            dma((nz - 1,)),
            dma((nz - 1,)),
            dma((nz - 1,)),
            dma((nz - 1,)),
            dma,
            dma,
            dma((groups, 2, nx)),
            dma((groups, 2, nx)),
            dma((nx,)),
            dma((nx,)),
            dma,
            dma,
            dma((groups, 2, nx)),
            dma((groups, nx)),
        ],
        compiler_params=pltpu.CompilerParams(
            collective_id=0, has_side_effects=True, vmem_limit_bytes=54500 * 1024
        ),
    )(small, hidden, w_query, w_latent, w_key, w_value, w_out)


def solution(mesh):
    return jax.shard_map(
        functools.partial(shards, mesh.shape["seq"], mesh.shape["head"]),
        mesh=mesh,
        in_specs=(
            P("rep", "seq", None),
            P("rep"),
            P("section", None),
            P("section", None, "head"),
            P("section", None, None),
            P("section", None),
            P("section", None, "head"),
            P("section", None, "head"),
            P("section", "head", None),
        ),
        out_specs=(P("rep", ("seq", "head"), "section"), P("section", "rep", "seq", None)),
        check_vma=False,
    )
```

```python
import functools

import jax
import jax.numpy as jnp
from jax import lax
from jax.experimental import pallas as pl
from jax.experimental.pallas import tpu as pltpu
from jax.sharding import PartitionSpec as P

HD = 128
EPS = 1e-06
NEG = -1e30
MESH = pl.DeviceIdType.MESH
LAST = (((1,), (1,)), ((), ()))


def rms_scale(values, gain):
    mean_sq = jnp.mean(values * values, axis=-1, keepdims=True)
    return values * lax.rsqrt(mean_sq + EPS) * gain


def dot(a, b):
    return jnp.dot(a, b, preferred_element_type=jnp.float32)


def dot_t(a, b):
    return lax.dot_general(a, b, LAST, preferred_element_type=jnp.float32)


def kernel(
    nz, nx, small, hid_hbm, wq_hbm, wl_hbm, wk_hbm, wv_hbm, wo_hbm,
    final, lat, counts, hid, wq, wl, wk, wv, wo, normed, kv, ownlat, absorbed, turned, last_keys, last_turned,
    top, total, accum, attn, part, headsum, xkeep, xhalf, finsum, load_sem,
    r_send, r_recv, l_send, l_recv, xa_send, xa_recv, xb_send, xb_recv, seed_send, seed_recv,
    sum_send, rs_recv, ag_send, ag_recv, half_send, half_recv, fin_recv,
):
    z, x, sec = lax.axis_index("seq"), lax.axis_index("head"), lax.axis_index("section")
    other = 1 - sec
    x_up, x_down = lax.rem(x + 1, nx), lax.rem(x + nx - 1, nx)
    groups, rows, width = hid.shape
    rank = wl.shape[1]
    heads = wk.shape[1] // HD
    share = rows // nx
    mine = groups * share
    half = width // 2
    mid = nz // 2
    levels = mid // 2
    hrows = heads * rows
    far_first = sorted(range(1, nx), key=lambda k: -min(k, nx - k))

    loads = [
        pltpu.make_async_copy(src, dst, load_sem.at[i])
        for i, (src, dst) in enumerate(
            [
                (hid_hbm, hid), (small.at[:, width + rank:], counts), (wl_hbm.at[0], wl),
                (wq_hbm.at[0], wq), (wk_hbm.at[0], wk), (wv_hbm.at[0], wv), (wo_hbm.at[0], wo),
            ]
        )
    ]
    for load in loads[:3]:
        load.start()

    main = mine - share
    for o in range(nx):
        kv[:, o, main:] = jnp.zeros((nz, share, rank), kv.dtype)

    barrier = pltpu.get_barrier_semaphore()
    peers = [{"seq": lax.rem(z + k, nz)} for k in (1, 2, nz - 2, nz - 1)]
    peers += [{"head": lax.rem(x + k, nx)} for k in range(1, nx)]
    peers += [{"section": other, "head": lax.rem(x + k, nx)} for k in range(nx)]
    for peer in peers:
        pl.semaphore_signal(barrier, inc=1, device_id=peer, device_id_type=MESH)

    def remote(src, dst, send, recv, to):
        return pltpu.make_async_remote_copy(
            src_ref=src, dst_ref=dst, send_sem=send, recv_sem=recv, device_id=to, device_id_type=MESH
        )

    def scatter_copy(b, h, owner, source):
        return remote(
            part.at[b, owner, h], headsum.at[source, b, h], sum_send.at[b, h, owner], rs_recv.at[b, h, source],
            {"section": other, "head": owner},
        )

    def normed_copy(to, source):
        return remote(normed.at[source], normed.at[source], ag_send.at[to], ag_recv.at[source], {"head": to})

    def half_copy():
        return remote(xkeep.at[0], xhalf, half_send, half_recv, {"section": other})

    def seed_copy(quarter):
        return remote(kv.at[z, quarter], kv.at[z, quarter], seed_send, seed_recv, {"head": x_down})

    def tile_left(d):
        return lax.rem(z + nz - d, nz)

    def tile_right(d):
        return lax.rem(z + d, nz)

    def either(carry, make, act):
        @pl.when(carry)
        def _():
            getattr(make(mine), act)()

        @pl.when(jnp.logical_not(carry))
        def _():
            getattr(make(main), act)()

    def right_copy(d, hop, q, act):
        tile = tile_left(d - hop)

        def make(count):
            spot = kv.at[tile, lax.rem(x + q, nx), pl.ds(0, count)]
            return remote(spot, spot, r_send.at[d - 1, q], r_recv.at[d - 1, q], {"seq": tile_right(hop)})

        either(tile + d < nz, make, act)

    def left_copy(d, hop, q, deep, act):
        tile = tile_right(d - hop)

        def make(count):
            spot = kv.at[tile, lax.rem(x + q, nx), pl.ds(0, count)]
            return remote(spot, spot, l_send.at[d - 1, q], l_recv.at[d - 1, q], {"seq": tile_left(hop)})

        either(tile < mid - 1 if deep else tile < d, make, act)

    def up_copy(tile, slot, quarter, act):
        def make(count):
            spot = kv.at[tile, quarter, pl.ds(0, count)]
            return remote(spot, spot, xa_send.at[slot], xa_recv.at[slot], {"head": x_up})

        either(tile <= z, make, act)

    def down_copy(tile, slot, quarter, act):
        def make(count):
            spot = kv.at[tile, quarter, pl.ds(0, count)]
            return remote(spot, spot, xb_send.at[slot], xb_recv.at[slot], {"head": x_down})

        either(tile <= z, make, act)

    def across(tile, slot, q):
        if q == 0:
            up_copy(tile, slot, x, "start")
        else:
            down_copy(tile, slot, x_up, "start")

    def await_across(tile, slot):
        up_copy(tile, slot, x_down, "wait_recv")
        down_copy(tile, slot, lax.rem(x + 2, nx), "wait_recv")

    def pieces(values):
        for o in range(nx):
            for b in range(groups):
                yield b, o, values[(o * groups + b) * share:(o * groups + b + 1) * share]

    def latents():
        flat = normed[...].reshape(nx * mine, width)
        full = rms_scale(dot(flat, wl[...]), lgain)
        for b, o, v in pieces(full):
            pos = z * rows + o * share + lax.broadcasted_iota(jnp.int32, (share, 1), 0)
            lat[0, b, o * share:(o + 1) * share] = jnp.where(pos < lengths[b], v, 0.0)
        return full.astype(jnp.bfloat16).reshape(nx, mine, rank)

    def normed_of(k):
        o = lax.rem(x + k, nx)
        at = pl.ds(pl.multiple_of(o * share, share), share)
        raw = jnp.concatenate([hid[b, at].astype(jnp.float32) for b in range(groups)], axis=0)
        normed[o] = rms_scale(raw, gain).astype(jnp.bfloat16)

    def fill_own():
        ownlat[...] = latents()
        for k in range(2, nx):
            o = lax.rem(x + k, nx)
            kv[z, o] = ownlat[o]

    gain, lgain = small[:, :width], small[:, width:width + rank]
    loads[0].wait()
    loads[1].wait()
    lengths = [counts[0, b].astype(jnp.int32) for b in range(groups)]

    @pl.when(sec == 0)
    def _():
        normed_of(0)
        normed_of(1)

    loads[2].wait()
    for load in loads[3:]:
        load.start()

    @pl.when(sec == 0)
    def _():
        rows_now = jnp.concatenate([normed[x], normed[x_up]], axis=0)
        early = rms_scale(dot(rows_now, wl[...]), lgain).astype(jnp.bfloat16)
        kv[z, x] = early[:mine]
        kv[z, x_up] = early[mine:]

    with jax.named_scope("barrier"):
        pl.semaphore_wait(barrier, len(peers))

    @pl.when(sec == 1)
    def _():
        for b in range(groups):
            with jax.named_scope("rswait"):
                for h in range(2):
                    for k in range(nx):
                        scatter_copy(b, h, x, k).wait_recv()
            at = pl.ds(b * share, share)
            own = hid[b, pl.ds(pl.multiple_of(x * share, share), share)].astype(jnp.float32)
            halves = []
            for h in range(2):
                add = headsum[0, b, h].astype(jnp.float32)
                for k in range(1, nx):
                    add = add + headsum[k, b, h].astype(jnp.float32)
                halves.append(own[:, h * half:(h + 1) * half] + add)
                xkeep[h, at] = halves[h]
            n = rms_scale(jnp.concatenate(halves, axis=1), gain)
            normed[x, at] = n.astype(jnp.bfloat16)
        early = rms_scale(dot(normed[x], wl[...]), lgain)
        kv[z, x] = early.astype(jnp.bfloat16)
        seed_copy(x).start()

    def first_sends(hop, q):
        right_copy(hop, hop, q, "start")
        left_copy(hop, hop, q, hop == 2, "start")

    @pl.when(sec == 0)
    def _():
        for hop in (2, 1):
            for q in range(2):
                first_sends(hop, q)

    @pl.when(sec == 1)
    def _():
        for hop in (2, 1):
            first_sends(hop, 0)
        for k in range(1, nx):
            normed_copy(lax.rem(x + k, nx), x).start()
        half_copy().start()
        with jax.named_scope("seedwait"):
            seed_copy(x_up).wait_recv()
        for hop in (2, 1):
            first_sends(hop, 1)

    def arrive(k):
        near, deep = 2 * k + 1, 2 * k + 2
        with jax.named_scope("zwait"):
            for q in range(2):
                right_copy(deep, 0, q, "wait_recv")

                @pl.when(k < levels - 1)
                def _():
                    right_copy(deep + 2, 2, q, "start")
                    left_copy(deep, 0, q, True, "wait_recv")

                @pl.when(k < levels - 2)
                def _():
                    left_copy(deep + 2, 2, q, True, "start")

            for q in range(2):

                @pl.when(k < levels - 1)
                def _():
                    right_copy(deep + 1, 1, q, "start")
                    left_copy(deep + 1, 1, q, False, "start")
                    across(tile_right(deep), mid + deep - 1, q)

                across(tile_left(deep), deep - 1, q)
            for q in range(2):
                right_copy(near, 0, q, "wait_recv")
                across(tile_left(near), near - 1, q)
                left_copy(near, 0, q, False, "wait_recv")
                across(tile_right(near), mid + near - 1, q)

    @pl.when(sec == 0)
    def _():
        with jax.named_scope("fill"):
            for k in range(2, nx):
                normed_of(k)
            fill_own()

    arrive(0)

    @pl.when(sec == 1)
    def _():
        with jax.named_scope("agwait"):
            for k in range(1, nx):
                normed_copy(x, lax.rem(x + k, nx)).wait_recv()
        fill_own()

    loads[3].wait()
    loads[4].wait()
    with jax.named_scope("query"):
        query = dot(normed[...].reshape(nx * mine, width), wq[...]).astype(jnp.bfloat16)
        for h in range(heads):
            cols = slice(h * HD, (h + 1) * HD)
            a = (dot_t(query[:, cols], wk[:, cols]) * (1.0 / HD**0.5)).astype(jnp.bfloat16)
            for b, o, v in pieces(a):
                absorbed[b, h * rows + o * share:h * rows + (o + 1) * share] = v
        for b in range(groups):
            turned[b] = absorbed[b].T

    key_at = lax.broadcasted_iota(jnp.int32, (rows, hrows), 0)
    row_at = lax.broadcasted_iota(jnp.int32, (rows, hrows), 1) % rows

    def gather_keys(tiles):
        keys = []
        for b in range(groups):
            for t in tiles:
                keys.append(kv[t, :, b * share:(b + 1) * share].reshape(rows, rank))
        keys = jnp.concatenate(keys, axis=0)
        return keys, keys.T

    def fold(qb, scores, keys_t, tiles, own, light):
        parts = []
        each = rows * len(tiles)
        blocks = qb if light else qb + 1
        for b in range(blocks):
            for i, t in enumerate(tiles):
                start = b * each + i * rows
                s = scores[start:start + rows]
                if b < qb:
                    seen = key_at < lengths[b] - t * rows
                elif own:
                    seen = key_at <= row_at
                else:
                    seen = key_at < jnp.where(t < z, rows, 0)
                parts.append(jnp.where(seen, s, NEG))
        scores = jnp.concatenate(parts, axis=0)
        peak = jnp.max(scores, axis=0, keepdims=True)
        if not own:
            old = top[qb]
            peak = jnp.maximum(old, peak)
            shrink = jnp.exp(old - peak)
        weights = jnp.exp(scores - peak)
        add = jnp.sum(weights, axis=0, keepdims=True)
        gained = dot(keys_t, weights.astype(jnp.bfloat16))
        if own:
            total[qb] = add
            accum[qb] = gained
        else:
            total[qb] = total[qb] * shrink + add
            accum[qb] = accum[qb] * shrink + gained
        top[qb] = peak

    def attend(tiles, own, light):
        keys, keys_t = gather_keys(tiles)
        each = rows * len(tiles)

        def count(qb):
            return (qb if light else qb + 1) * each

        start = 1 if light else 0
        ahead = dot(keys[:count(start)], turned[start])
        for qb in range(start, groups):
            now = ahead
            if qb + 1 < groups:
                ahead = dot(keys[:count(qb + 1)], turned[qb + 1])
            fold(qb, now, keys_t[:, :count(qb)], tiles, own, light)

    with jax.named_scope("attend_own"):
        attend([z], True, False)

    def level(k, carry):
        arrive(k)

        def pair(d, c):
            with jax.named_scope("xwait"):
                await_across(tile_left(d), d - 1)
                await_across(tile_right(d), mid + d - 1)
            light = jnp.logical_and(z < d, z + d < nz)

            @pl.when(light)
            def _():
                with jax.named_scope("attend_light"):
                    attend([tile_left(d), tile_right(d)], False, True)

            @pl.when(jnp.logical_not(light))
            def _():
                with jax.named_scope("attend_pair"):
                    attend([tile_left(d), tile_right(d)], False, False)

            return c

        lax.fori_loop(2 * k - 1, 2 * k + 1, pair, 0)
        return carry

    lax.fori_loop(1, levels, level, 0)
    ends = [tile_left(mid - 1), tile_right(mid - 1), tile_left(mid)]
    with jax.named_scope("farwait"):
        await_across(ends[0], mid - 2)
        await_across(ends[1], 2 * mid - 2)
        await_across(ends[2], mid - 1)
    end_keys, end_turned = gather_keys(ends)
    last_keys[...] = end_keys
    last_turned[...] = end_turned
    all_later = z < mid - 1

    for load in loads[5:]:
        load.wait()

    def finish_copy(b, h, owner, source):
        return remote(
            part.at[b, owner, h], finsum.at[source, b], sum_send.at[b, h, owner], fin_recv.at[b, source],
            {"section": h, "head": owner},
        )

    for b in range(groups):

        def last_fold(light):
            n = (b if light else b + 1) * len(ends) * rows
            fold(b, dot(last_keys[:n], turned[b]), last_turned[:, :n], ends, False, light)

        with jax.named_scope("attend_last"):
            if b > 0:

                @pl.when(all_later)
                def _():
                    last_fold(True)

            @pl.when(jnp.logical_not(all_later))
            def _():
                last_fold(False)

        with jax.named_scope("project"):
            context = (accum[b] / total[b]).astype(jnp.bfloat16).T
            for h in range(heads):
                cols = slice(h * HD, (h + 1) * HD)
                attn[:, cols] = dot(context[h * rows:(h + 1) * rows], wv[:, cols]).astype(jnp.bfloat16)
        for h in range(2):
            with jax.named_scope("out"):
                out = dot(attn[...], wo[:, h * half:(h + 1) * half]).astype(jnp.bfloat16)
                for o in range(nx):
                    part[b, o, h] = out[o * share:(o + 1) * share]

            @pl.when(sec == 0)
            def _():
                for k in far_first + [0]:
                    scatter_copy(b, h, lax.rem(x + k, nx), x).start()

            @pl.when(sec == 1)
            def _():
                for k in far_first + [0] * (1 - h):
                    finish_copy(b, h, lax.rem(x + k, nx), x).start()

    def drain(k, carry):
        for d, hop in ((2 * k + 1, 1), (2 * k + 2, 2)):
            for q in range(2):
                right_copy(d, hop, q, "wait_send")
            up_copy(tile_left(d), d - 1, x, "wait_send")
            down_copy(tile_left(d), d - 1, x, "wait_send")

            @pl.when(d < mid)
            def _():
                for q in range(2):
                    left_copy(d, hop, q, hop == 2, "wait_send")
                up_copy(tile_right(d), mid + d - 1, x, "wait_send")
                down_copy(tile_right(d), mid + d - 1, x, "wait_send")

        return carry

    with jax.named_scope("drain"):
        lax.fori_loop(0, levels, drain, 0)

    @pl.when(sec == 0)
    def _():
        half_copy().wait_recv()
        for b in range(groups):
            for h in range(2):
                for o in range(nx):
                    scatter_copy(b, h, o, x).wait_send()

    @pl.when(sec == 1)
    def _():
        xhalf[...] = xkeep[1]
        half_copy().wait_send()
        seed_copy(x).wait_send()
        for k in range(1, nx):
            normed_copy(lax.rem(x + k, nx), x).wait_send()

    for b in range(groups):

        @pl.when(sec == 0)
        def _():
            with jax.named_scope("finwait0"):
                for k in range(nx):
                    finish_copy(b, 0, x, k).wait_recv()

        @pl.when(sec == 1)
        def _():
            finsum[x, b] = part[b, x, 1]
            with jax.named_scope("finwait1"):
                for k in range(1, nx):
                    finish_copy(b, 1, x, lax.rem(x + k, nx)).wait_recv()

        at = pl.ds(b * share, share)
        add = finsum[0, b].astype(jnp.float32)
        for k in range(1, nx):
            add = add + finsum[k, b].astype(jnp.float32)
        pos = z * rows + x * share + lax.broadcasted_iota(jnp.int32, (share, 1), 0)
        final[b] = jnp.where(pos < lengths[b], xhalf[at] + add, 0.0)

    @pl.when(sec == 1)
    def _():
        for b in range(groups):
            for k in range(1, nx):
                for h in range(2):
                    finish_copy(b, h, lax.rem(x + k, nx), x).wait_send()
            finish_copy(b, 0, x, x).wait_send()


def shards(nz, nx, hidden, lengths, attn_gain, w_query, w_latent, latent_gain, w_key, w_value, w_out):
    groups, rows, width = hidden.shape
    rank = w_latent.shape[2]
    cols = w_key.shape[2]
    heads = cols // HD
    share = rows // nx
    mine = groups * share
    half = width // 2
    mid = nz // 2
    vmem, dma = pltpu.VMEM, pltpu.SemaphoreType.DMA
    whole = pl.BlockSpec(memory_space=pltpu.VMEM)
    hbm = pl.BlockSpec(memory_space=pl.ANY)
    bf16, f32 = jnp.bfloat16, jnp.float32
    flat = ((0, 0, 0),)
    pieces = (attn_gain, latent_gain, lengths[None])
    size, at, small = width + rank + 128, 0, 0.0
    for piece in pieces:
        count = piece.shape[1]
        zero = jnp.zeros((), piece.dtype)
        small = small + lax.pad(piece, zero, flat + ((at, size - at - count, 0),)).astype(f32)
        at += count
    return pl.pallas_call(
        functools.partial(kernel, nz, nx),
        out_shape=(
            jax.ShapeDtypeStruct((groups, share, half), f32),
            jax.ShapeDtypeStruct((1, groups, rows, rank), f32),
        ),
        in_specs=[whole] + [hbm] * 6,
        out_specs=(whole, whole),
        scratch_shapes=[
            pltpu.SMEM((1, 128), f32),
            vmem((groups, rows, width), bf16),
            vmem((width, cols), bf16),
            vmem((width, rank), bf16),
            vmem((rank, cols), bf16),
            vmem((rank, cols), bf16),
            vmem((cols, width), bf16),
            vmem((nx, mine, width), bf16),
            vmem((nz, nx, mine, rank), bf16),
            vmem((nx, mine, rank), bf16),
            vmem((groups, heads * rows, rank), bf16),
            vmem((groups, rank, heads * rows), bf16),
            vmem((3 * groups * rows, rank), bf16),
            vmem((rank, 3 * groups * rows), bf16),
            vmem((groups, 1, heads * rows), f32),
            vmem((groups, 1, heads * rows), f32),
            vmem((groups, rank, heads * rows), f32),
            vmem((rows, cols), bf16),
            vmem((groups, nx, 2, share, half), bf16),
            vmem((nx, groups, 2, share, half), bf16),
            vmem((2, mine, half), f32),
            vmem((mine, half), f32),
            vmem((nx, groups, share, half), bf16),
            dma((7,)),
            dma((mid, 2)),
            dma((mid, 2)),
            dma((mid, 2)),
            dma((mid, 2)),
            dma((nz - 1,)),
            dma((nz - 1,)),
            dma((nz - 1,)),
            dma((nz - 1,)),
            dma,
            dma,
            dma((groups, 2, nx)),
            dma((groups, 2, nx)),
            dma((nx,)),
            dma((nx,)),
            dma,
            dma,
            dma((groups, nx)),
        ],
        compiler_params=pltpu.CompilerParams(
            collective_id=0, has_side_effects=True, vmem_limit_bytes=54500 * 1024
        ),
    )(small, hidden, w_query, w_latent, w_key, w_value, w_out)


def solution(mesh):
    return jax.shard_map(
        functools.partial(shards, mesh.shape["seq"], mesh.shape["head"]),
        mesh=mesh,
        in_specs=(
            P("rep", "seq", None),
            P("rep"),
            P("section", None),
            P("section", None, "head"),
            P("section", None, None),
            P("section", None),
            P("section", None, "head"),
            P("section", None, "head"),
            P("section", "head", None),
        ),
        out_specs=(P("rep", ("seq", "head"), "section"), P("section", "rep", "seq", None)),
        check_vma=False,
    )
```

```python
import functools

import jax
import jax.numpy as jnp
from jax import lax
from jax.experimental import pallas as pl
from jax.experimental.pallas import tpu as pltpu
from jax.sharding import PartitionSpec as P

HD = 128
EPS = 1e-06
NEG = -1e30
MESH = pl.DeviceIdType.MESH
LAST = (((1,), (1,)), ((), ()))


def rms_scale(values, gain):
    mean_sq = jnp.mean(values * values, axis=-1, keepdims=True)
    return values * lax.rsqrt(mean_sq + EPS) * gain


def dot(a, b):
    return jnp.dot(a, b, preferred_element_type=jnp.float32)


def dot_t(a, b):
    return lax.dot_general(a, b, LAST, preferred_element_type=jnp.float32)


def kernel(
    nz, nx, small, hid_hbm, wq_hbm, wl_hbm, wk_hbm, wv_hbm, wo_hbm,
    final, lat, counts, hid, wq, wl, wk, wv, wo, normed, kv, ownlat, absorbed, turned, last_keys, last_turned,
    top, total, accum, attn, part, headsum, xkeep, xhalf, finsum, load_sem,
    r_send, r_recv, l_send, l_recv, xa_send, xa_recv, xb_send, xb_recv, seed_send, seed_recv,
    sum_send, rs_recv, ag_send, ag_recv, half_send, half_recv, fin_recv,
):
    z, x, sec = lax.axis_index("seq"), lax.axis_index("head"), lax.axis_index("section")
    other = 1 - sec
    x_up, x_down = lax.rem(x + 1, nx), lax.rem(x + nx - 1, nx)
    groups, rows, width = hid.shape
    rank = wl.shape[1]
    heads = wk.shape[1] // HD
    share = rows // nx
    mine = groups * share
    half = width // 2
    mid = nz // 2
    levels = mid // 2
    hrows = heads * rows
    far_first = sorted(range(1, nx), key=lambda k: -min(k, nx - k))

    loads = [
        pltpu.make_async_copy(src, dst, load_sem.at[i])
        for i, (src, dst) in enumerate(
            [
                (hid_hbm, hid), (small.at[:, width + rank:], counts), (wl_hbm.at[0], wl),
                (wq_hbm.at[0], wq), (wk_hbm.at[0], wk), (wv_hbm.at[0], wv), (wo_hbm.at[0], wo),
            ]
        )
    ]
    for load in loads[:3]:
        load.start()

    main = mine - share
    for o in range(nx):
        kv[:, o, main:] = jnp.zeros((nz, share, rank), kv.dtype)

    barrier = pltpu.get_barrier_semaphore()
    peers = [{"seq": lax.rem(z + k, nz)} for k in (1, 2, nz - 2, nz - 1)]
    peers += [{"head": lax.rem(x + k, nx)} for k in range(1, nx)]
    peers += [{"section": other, "head": lax.rem(x + k, nx)} for k in range(nx)]
    for peer in peers:
        pl.semaphore_signal(barrier, inc=1, device_id=peer, device_id_type=MESH)

    def remote(src, dst, send, recv, to):
        return pltpu.make_async_remote_copy(
            src_ref=src, dst_ref=dst, send_sem=send, recv_sem=recv, device_id=to, device_id_type=MESH
        )

    def scatter_copy(b, h, owner, source):
        return remote(
            part.at[b, owner, h], headsum.at[source, b, h], sum_send.at[b, h, owner], rs_recv.at[b, h, source],
            {"section": other, "head": owner},
        )

    def normed_copy(b, to, source):
        spot = normed.at[source, pl.ds(b * share, share)]
        return remote(spot, spot, ag_send.at[b, to], ag_recv.at[b, source], {"head": to})

    def half_copy():
        return remote(xkeep.at[0], xhalf, half_send, half_recv, {"section": other})

    def seed_copy(quarter):
        return remote(kv.at[z, quarter], kv.at[z, quarter], seed_send, seed_recv, {"head": x_down})

    def tile_left(d):
        return lax.rem(z + nz - d, nz)

    def tile_right(d):
        return lax.rem(z + d, nz)

    def either(carry, make, act):
        @pl.when(carry)
        def _():
            getattr(make(mine), act)()

        @pl.when(jnp.logical_not(carry))
        def _():
            getattr(make(main), act)()

    def right_copy(d, hop, q, act):
        tile = tile_left(d - hop)

        def make(count):
            spot = kv.at[tile, lax.rem(x + q, nx), pl.ds(0, count)]
            return remote(spot, spot, r_send.at[d - 1, q], r_recv.at[d - 1, q], {"seq": tile_right(hop)})

        either(tile + d < nz, make, act)

    def left_copy(d, hop, q, deep, act):
        tile = tile_right(d - hop)

        def make(count):
            spot = kv.at[tile, lax.rem(x + q, nx), pl.ds(0, count)]
            return remote(spot, spot, l_send.at[d - 1, q], l_recv.at[d - 1, q], {"seq": tile_left(hop)})

        either(tile < mid - 1 if deep else tile < d, make, act)

    def up_copy(tile, slot, quarter, act):
        def make(count):
            spot = kv.at[tile, quarter, pl.ds(0, count)]
            return remote(spot, spot, xa_send.at[slot], xa_recv.at[slot], {"head": x_up})

        either(tile <= z, make, act)

    def down_copy(tile, slot, quarter, act):
        def make(count):
            spot = kv.at[tile, quarter, pl.ds(0, count)]
            return remote(spot, spot, xb_send.at[slot], xb_recv.at[slot], {"head": x_down})

        either(tile <= z, make, act)

    def across(tile, slot, q):
        if q == 0:
            up_copy(tile, slot, x, "start")
        else:
            down_copy(tile, slot, x_up, "start")

    def await_across(tile, slot):
        up_copy(tile, slot, x_down, "wait_recv")
        down_copy(tile, slot, lax.rem(x + 2, nx), "wait_recv")

    def pieces(values):
        for o in range(nx):
            for b in range(groups):
                yield b, o, values[(o * groups + b) * share:(o * groups + b + 1) * share]

    def latents():
        flat = normed[...].reshape(nx * mine, width)
        full = rms_scale(dot(flat, wl[...]), lgain)
        for b, o, v in pieces(full):
            pos = z * rows + o * share + lax.broadcasted_iota(jnp.int32, (share, 1), 0)
            lat[0, b, o * share:(o + 1) * share] = jnp.where(pos < lengths[b], v, 0.0)
        return full.astype(jnp.bfloat16).reshape(nx, mine, rank)

    def normed_of(k):
        o = lax.rem(x + k, nx)
        at = pl.ds(pl.multiple_of(o * share, share), share)
        raw = jnp.concatenate([hid[b, at].astype(jnp.float32) for b in range(groups)], axis=0)
        normed[o] = rms_scale(raw, gain).astype(jnp.bfloat16)

    def fill_own():
        ownlat[...] = latents()
        for k in range(2, nx):
            o = lax.rem(x + k, nx)
            kv[z, o] = ownlat[o]

    gain, lgain = small[:, :width], small[:, width:width + rank]
    loads[0].wait()
    loads[1].wait()
    lengths = [counts[0, b].astype(jnp.int32) for b in range(groups)]

    @pl.when(sec == 0)
    def _():
        normed_of(0)
        normed_of(1)

    loads[2].wait()
    for load in loads[3:]:
        load.start()

    @pl.when(sec == 0)
    def _():
        rows_now = jnp.concatenate([normed[x], normed[x_up]], axis=0)
        early = rms_scale(dot(rows_now, wl[...]), lgain).astype(jnp.bfloat16)
        kv[z, x] = early[:mine]
        kv[z, x_up] = early[mine:]

    with jax.named_scope("barrier"):
        pl.semaphore_wait(barrier, len(peers))

    @pl.when(sec == 1)
    def _():
        for b in range(groups):
            with jax.named_scope("rswait"):
                for h in range(2):
                    for k in range(nx):
                        scatter_copy(b, h, x, k).wait_recv()
            at = pl.ds(b * share, share)
            own = hid[b, pl.ds(pl.multiple_of(x * share, share), share)].astype(jnp.float32)
            halves = []
            for h in range(2):
                add = headsum[0, b, h].astype(jnp.float32)
                for k in range(1, nx):
                    add = add + headsum[k, b, h].astype(jnp.float32)
                halves.append(own[:, h * half:(h + 1) * half] + add)
                xkeep[h, at] = halves[h]
            n = rms_scale(jnp.concatenate(halves, axis=1), gain)
            normed[x, at] = n.astype(jnp.bfloat16)
            if b + 1 < groups:
                for k in far_first:
                    normed_copy(b, lax.rem(x + k, nx), x).start()
        early = rms_scale(dot(normed[x], wl[...]), lgain)
        kv[z, x] = early.astype(jnp.bfloat16)
        seed_copy(x).start()

    def first_sends(hop, q):
        right_copy(hop, hop, q, "start")
        left_copy(hop, hop, q, hop == 2, "start")

    @pl.when(sec == 0)
    def _():
        for hop in (2, 1):
            for q in range(2):
                first_sends(hop, q)

    @pl.when(sec == 1)
    def _():
        for hop in (2, 1):
            first_sends(hop, 0)
        for k in far_first:
            normed_copy(groups - 1, lax.rem(x + k, nx), x).start()
        half_copy().start()
        with jax.named_scope("seedwait"):
            seed_copy(x_up).wait_recv()
        for hop in (2, 1):
            first_sends(hop, 1)

    def arrive(k):
        near, deep = 2 * k + 1, 2 * k + 2
        with jax.named_scope("zwait"):
            for q in range(2):
                right_copy(deep, 0, q, "wait_recv")

                @pl.when(k < levels - 1)
                def _():
                    right_copy(deep + 2, 2, q, "start")
                    left_copy(deep, 0, q, True, "wait_recv")

                @pl.when(k < levels - 2)
                def _():
                    left_copy(deep + 2, 2, q, True, "start")

            for q in range(2):

                @pl.when(k < levels - 1)
                def _():
                    right_copy(deep + 1, 1, q, "start")
                    left_copy(deep + 1, 1, q, False, "start")
                    across(tile_right(deep), mid + deep - 1, q)

                across(tile_left(deep), deep - 1, q)
            for q in range(2):
                right_copy(near, 0, q, "wait_recv")
                across(tile_left(near), near - 1, q)
                left_copy(near, 0, q, False, "wait_recv")
                across(tile_right(near), mid + near - 1, q)

    @pl.when(sec == 0)
    def _():
        with jax.named_scope("fill"):
            for k in range(2, nx):
                normed_of(k)
            fill_own()

    @pl.when(sec == 1)
    def _():
        with jax.named_scope("agwait"):
            for b in range(groups):
                for k in range(1, nx):
                    normed_copy(b, x, lax.rem(x + k, nx)).wait_recv()

    loads[3].wait()
    loads[4].wait()
    with jax.named_scope("query"):
        query = dot(normed[...].reshape(nx * mine, width), wq[...]).astype(jnp.bfloat16)
        for h in range(heads):
            cols = slice(h * HD, (h + 1) * HD)
            a = (dot_t(query[:, cols], wk[:, cols]) * (1.0 / HD**0.5)).astype(jnp.bfloat16)
            for b, o, v in pieces(a):
                absorbed[b, h * rows + o * share:h * rows + (o + 1) * share] = v
        for b in range(groups):
            turned[b] = absorbed[b].T

    arrive(0)

    @pl.when(sec == 1)
    def _():
        with jax.named_scope("fill"):
            fill_own()

    key_at = lax.broadcasted_iota(jnp.int32, (rows, hrows), 0)
    row_at = lax.broadcasted_iota(jnp.int32, (rows, hrows), 1) % rows

    def gather_keys(tiles):
        keys = []
        for b in range(groups):
            for t in tiles:
                keys.append(kv[t, :, b * share:(b + 1) * share].reshape(rows, rank))
        keys = jnp.concatenate(keys, axis=0)
        return keys, keys.T

    def fold(qb, scores, keys_t, tiles, own, light):
        parts = []
        each = rows * len(tiles)
        blocks = qb if light else qb + 1
        for b in range(blocks):
            for i, t in enumerate(tiles):
                start = b * each + i * rows
                s = scores[start:start + rows]
                if b < qb:
                    seen = key_at < lengths[b] - t * rows
                elif own:
                    seen = key_at <= row_at
                else:
                    seen = key_at < jnp.where(t < z, rows, 0)
                parts.append(jnp.where(seen, s, NEG))
        scores = jnp.concatenate(parts, axis=0)
        peak = jnp.max(scores, axis=0, keepdims=True)
        if not own:
            old = top[qb]
            peak = jnp.maximum(old, peak)
            shrink = jnp.exp(old - peak)
        weights = jnp.exp(scores - peak)
        add = jnp.sum(weights, axis=0, keepdims=True)
        gained = dot(keys_t, weights.astype(jnp.bfloat16))
        if own:
            total[qb] = add
            accum[qb] = gained
        else:
            total[qb] = total[qb] * shrink + add
            accum[qb] = accum[qb] * shrink + gained
        top[qb] = peak

    def attend(tiles, own, light):
        keys, keys_t = gather_keys(tiles)
        each = rows * len(tiles)

        def count(qb):
            return (qb if light else qb + 1) * each

        start = 1 if light else 0
        ahead = dot(keys[:count(start)], turned[start])
        for qb in range(start, groups):
            now = ahead
            if qb + 1 < groups:
                ahead = dot(keys[:count(qb + 1)], turned[qb + 1])
            fold(qb, now, keys_t[:, :count(qb)], tiles, own, light)

    with jax.named_scope("attend_own"):
        attend([z], True, False)

    def level(k, carry):
        arrive(k)

        def pair(d, c):
            with jax.named_scope("xwait"):
                await_across(tile_left(d), d - 1)
                await_across(tile_right(d), mid + d - 1)
            light = jnp.logical_and(z < d, z + d < nz)

            @pl.when(light)
            def _():
                with jax.named_scope("attend_light"):
                    attend([tile_left(d), tile_right(d)], False, True)

            @pl.when(jnp.logical_not(light))
            def _():
                with jax.named_scope("attend_pair"):
                    attend([tile_left(d), tile_right(d)], False, False)

            return c

        lax.fori_loop(2 * k - 1, 2 * k + 1, pair, 0)
        return carry

    lax.fori_loop(1, levels, level, 0)
    ends = [tile_left(mid - 1), tile_right(mid - 1), tile_left(mid)]
    with jax.named_scope("farwait"):
        await_across(ends[0], mid - 2)
        await_across(ends[1], 2 * mid - 2)
        await_across(ends[2], mid - 1)
    end_keys, end_turned = gather_keys(ends)
    last_keys[...] = end_keys
    last_turned[...] = end_turned
    all_later = z < mid - 1

    for load in loads[5:]:
        load.wait()

    def finish_copy(b, h, owner, source):
        return remote(
            part.at[b, owner, h], finsum.at[source, b], sum_send.at[b, h, owner], fin_recv.at[b, source],
            {"section": h, "head": owner},
        )

    for b in range(groups):

        def last_fold(light):
            n = (b if light else b + 1) * len(ends) * rows
            fold(b, dot(last_keys[:n], turned[b]), last_turned[:, :n], ends, False, light)

        with jax.named_scope("attend_last"):
            if b > 0:

                @pl.when(all_later)
                def _():
                    last_fold(True)

            @pl.when(jnp.logical_not(all_later))
            def _():
                last_fold(False)

        with jax.named_scope("project"):
            context = (accum[b] / total[b]).astype(jnp.bfloat16).T
            for h in range(heads):
                cols = slice(h * HD, (h + 1) * HD)
                attn[:, cols] = dot(context[h * rows:(h + 1) * rows], wv[:, cols]).astype(jnp.bfloat16)
        for h in range(2):
            with jax.named_scope("out"):
                out = dot(attn[...], wo[:, h * half:(h + 1) * half]).astype(jnp.bfloat16)
                for o in range(nx):
                    part[b, o, h] = out[o * share:(o + 1) * share]

            @pl.when(sec == 0)
            def _():
                for k in far_first + [0]:
                    scatter_copy(b, h, lax.rem(x + k, nx), x).start()

            @pl.when(sec == 1)
            def _():
                for k in far_first + [0] * (1 - h):
                    finish_copy(b, h, lax.rem(x + k, nx), x).start()

    def drain(k, carry):
        for d, hop in ((2 * k + 1, 1), (2 * k + 2, 2)):
            for q in range(2):
                right_copy(d, hop, q, "wait_send")
            up_copy(tile_left(d), d - 1, x, "wait_send")
            down_copy(tile_left(d), d - 1, x, "wait_send")

            @pl.when(d < mid)
            def _():
                for q in range(2):
                    left_copy(d, hop, q, hop == 2, "wait_send")
                up_copy(tile_right(d), mid + d - 1, x, "wait_send")
                down_copy(tile_right(d), mid + d - 1, x, "wait_send")

        return carry

    with jax.named_scope("drain"):
        lax.fori_loop(0, levels, drain, 0)

    @pl.when(sec == 0)
    def _():
        half_copy().wait_recv()
        for b in range(groups):
            for h in range(2):
                for o in range(nx):
                    scatter_copy(b, h, o, x).wait_send()

    @pl.when(sec == 1)
    def _():
        xhalf[...] = xkeep[1]
        half_copy().wait_send()
        seed_copy(x).wait_send()
        for b in range(groups):
            for k in range(1, nx):
                normed_copy(b, lax.rem(x + k, nx), x).wait_send()

    for b in range(groups):

        @pl.when(sec == 0)
        def _():
            with jax.named_scope("finwait0"):
                for k in range(nx):
                    finish_copy(b, 0, x, k).wait_recv()

        @pl.when(sec == 1)
        def _():
            finsum[x, b] = part[b, x, 1]
            with jax.named_scope("finwait1"):
                for k in range(1, nx):
                    finish_copy(b, 1, x, lax.rem(x + k, nx)).wait_recv()

        at = pl.ds(b * share, share)
        add = finsum[0, b].astype(jnp.float32)
        for k in range(1, nx):
            add = add + finsum[k, b].astype(jnp.float32)
        pos = z * rows + x * share + lax.broadcasted_iota(jnp.int32, (share, 1), 0)
        final[b] = jnp.where(pos < lengths[b], xhalf[at] + add, 0.0)

    @pl.when(sec == 1)
    def _():
        for b in range(groups):
            for k in range(1, nx):
                for h in range(2):
                    finish_copy(b, h, lax.rem(x + k, nx), x).wait_send()
            finish_copy(b, 0, x, x).wait_send()


def shards(nz, nx, hidden, lengths, attn_gain, w_query, w_latent, latent_gain, w_key, w_value, w_out):
    groups, rows, width = hidden.shape
    rank = w_latent.shape[2]
    cols = w_key.shape[2]
    heads = cols // HD
    share = rows // nx
    mine = groups * share
    half = width // 2
    mid = nz // 2
    vmem, dma = pltpu.VMEM, pltpu.SemaphoreType.DMA
    whole = pl.BlockSpec(memory_space=pltpu.VMEM)
    hbm = pl.BlockSpec(memory_space=pl.ANY)
    bf16, f32 = jnp.bfloat16, jnp.float32
    flat = ((0, 0, 0),)
    pieces = (attn_gain, latent_gain, lengths[None])
    size, at, small = width + rank + 128, 0, 0.0
    for piece in pieces:
        count = piece.shape[1]
        zero = jnp.zeros((), piece.dtype)
        small = small + lax.pad(piece, zero, flat + ((at, size - at - count, 0),)).astype(f32)
        at += count
    return pl.pallas_call(
        functools.partial(kernel, nz, nx),
        out_shape=(
            jax.ShapeDtypeStruct((groups, share, half), f32),
            jax.ShapeDtypeStruct((1, groups, rows, rank), f32),
        ),
        in_specs=[whole] + [hbm] * 6,
        out_specs=(whole, whole),
        scratch_shapes=[
            pltpu.SMEM((1, 128), f32),
            vmem((groups, rows, width), bf16),
            vmem((width, cols), bf16),
            vmem((width, rank), bf16),
            vmem((rank, cols), bf16),
            vmem((rank, cols), bf16),
            vmem((cols, width), bf16),
            vmem((nx, mine, width), bf16),
            vmem((nz, nx, mine, rank), bf16),
            vmem((nx, mine, rank), bf16),
            vmem((groups, heads * rows, rank), bf16),
            vmem((groups, rank, heads * rows), bf16),
            vmem((3 * groups * rows, rank), bf16),
            vmem((rank, 3 * groups * rows), bf16),
            vmem((groups, 1, heads * rows), f32),
            vmem((groups, 1, heads * rows), f32),
            vmem((groups, rank, heads * rows), f32),
            vmem((rows, cols), bf16),
            vmem((groups, nx, 2, share, half), bf16),
            vmem((nx, groups, 2, share, half), bf16),
            vmem((2, mine, half), f32),
            vmem((mine, half), f32),
            vmem((nx, groups, share, half), bf16),
            dma((7,)),
            dma((mid, 2)),
            dma((mid, 2)),
            dma((mid, 2)),
            dma((mid, 2)),
            dma((nz - 1,)),
            dma((nz - 1,)),
            dma((nz - 1,)),
            dma((nz - 1,)),
            dma,
            dma,
            dma((groups, 2, nx)),
            dma((groups, 2, nx)),
            dma((groups, nx)),
            dma((groups, nx)),
            dma,
            dma,
            dma((groups, nx)),
        ],
        compiler_params=pltpu.CompilerParams(
            collective_id=0, has_side_effects=True, vmem_limit_bytes=54500 * 1024
        ),
    )(small, hidden, w_query, w_latent, w_key, w_value, w_out)


def solution(mesh):
    return jax.shard_map(
        functools.partial(shards, mesh.shape["seq"], mesh.shape["head"]),
        mesh=mesh,
        in_specs=(
            P("rep", "seq", None),
            P("rep"),
            P("section", None),
            P("section", None, "head"),
            P("section", None, None),
            P("section", None),
            P("section", None, "head"),
            P("section", None, "head"),
            P("section", "head", None),
        ),
        out_specs=(P("rep", ("seq", "head"), "section"), P("section", "rep", "seq", None)),
        check_vma=False,
    )
```

```python
import functools

import jax
import jax.numpy as jnp
from jax import lax
from jax.experimental import pallas as pl
from jax.experimental.pallas import tpu as pltpu
from jax.sharding import PartitionSpec as P

HD = 128
EPS = 1e-06
NEG = -1e30
MESH = pl.DeviceIdType.MESH
LAST = (((1,), (1,)), ((), ()))


def rms_scale(values, gain):
    mean_sq = jnp.mean(values * values, axis=-1, keepdims=True)
    return values * lax.rsqrt(mean_sq + EPS) * gain


def dot(a, b):
    return jnp.dot(a, b, preferred_element_type=jnp.float32)


def dot_t(a, b):
    return lax.dot_general(a, b, LAST, preferred_element_type=jnp.float32)


def kernel(
    nz, nx, small, hid_hbm, wq_hbm, wl_hbm, wk_hbm, wv_hbm, wo_hbm,
    final, lat, counts, hid, wq, wl, wk, wv, wo, normed, kv, ownlat, absorbed, turned, last_keys, last_turned,
    top, total, accum, attn, part, headsum, xkeep, xhalf, finsum, load_sem,
    r_send, r_recv, l_send, l_recv, xa_send, xa_recv, xb_send, xb_recv, seed_send, seed_recv,
    sum_send, rs_recv, ag_send, ag_recv, half_send, half_recv, fin_recv,
):
    z, x, sec = lax.axis_index("seq"), lax.axis_index("head"), lax.axis_index("section")
    other = 1 - sec
    x_up, x_down = lax.rem(x + 1, nx), lax.rem(x + nx - 1, nx)
    groups, rows, width = hid.shape
    rank = wl.shape[1]
    heads = wk.shape[1] // HD
    share = rows // nx
    mine = groups * share
    half = width // 2
    mid = nz // 2
    levels = mid // 2
    hrows = heads * rows
    far_first = sorted(range(1, nx), key=lambda k: -min(k, nx - k))

    cut = width // 4
    moves = [(hid_hbm.at[b], hid.at[b]) for b in range(groups)]
    moves += [(small.at[:, width + rank:], counts)]
    moves += [(wl_hbm.at[0, pl.ds(i * cut, cut)], wl.at[pl.ds(i * cut, cut)]) for i in range(4)]
    moves += [(wq_hbm.at[0], wq), (wk_hbm.at[0], wk), (wv_hbm.at[0], wv), (wo_hbm.at[0], wo)]
    loads = [pltpu.make_async_copy(src, dst, load_sem.at[i]) for i, (src, dst) in enumerate(moves)]
    latent_at = groups + 1
    rest_at = latent_at + 4
    for load in loads[:rest_at]:
        load.start()

    main = mine - share
    for o in range(nx):
        kv[:, o, main:] = jnp.zeros((nz, share, rank), kv.dtype)

    barrier = pltpu.get_barrier_semaphore()
    peers = [{"seq": lax.rem(z + k, nz)} for k in (1, 2, nz - 2, nz - 1)]
    peers += [{"head": lax.rem(x + k, nx)} for k in range(1, nx)]
    peers += [{"section": other, "head": lax.rem(x + k, nx)} for k in range(nx)]
    for peer in peers:
        pl.semaphore_signal(barrier, inc=1, device_id=peer, device_id_type=MESH)

    def remote(src, dst, send, recv, to):
        return pltpu.make_async_remote_copy(
            src_ref=src, dst_ref=dst, send_sem=send, recv_sem=recv, device_id=to, device_id_type=MESH
        )

    def scatter_copy(b, h, owner, source):
        return remote(
            part.at[b, owner, h], headsum.at[source, b, h], sum_send.at[b, h, owner], rs_recv.at[b, h, source],
            {"section": other, "head": owner},
        )

    def normed_copy(to, source):
        return remote(normed.at[source], normed.at[source], ag_send.at[to], ag_recv.at[source], {"head": to})

    def half_copy():
        return remote(xkeep.at[0], xhalf, half_send, half_recv, {"section": other})

    def seed_copy(quarter):
        return remote(kv.at[z, quarter], kv.at[z, quarter], seed_send, seed_recv, {"head": x_down})

    def tile_left(d):
        return lax.rem(z + nz - d, nz)

    def tile_right(d):
        return lax.rem(z + d, nz)

    def either(carry, make, act):
        @pl.when(carry)
        def _():
            getattr(make(mine), act)()

        @pl.when(jnp.logical_not(carry))
        def _():
            getattr(make(main), act)()

    def right_copy(d, hop, q, act):
        tile = tile_left(d - hop)

        def make(count):
            spot = kv.at[tile, lax.rem(x + q, nx), pl.ds(0, count)]
            return remote(spot, spot, r_send.at[d - 1, q], r_recv.at[d - 1, q], {"seq": tile_right(hop)})

        either(tile + d < nz, make, act)

    def left_copy(d, hop, q, deep, act):
        tile = tile_right(d - hop)

        def make(count):
            spot = kv.at[tile, lax.rem(x + q, nx), pl.ds(0, count)]
            return remote(spot, spot, l_send.at[d - 1, q], l_recv.at[d - 1, q], {"seq": tile_left(hop)})

        either(tile < mid - 1 if deep else tile < d, make, act)

    def up_copy(tile, slot, quarter, act):
        def make(count):
            spot = kv.at[tile, quarter, pl.ds(0, count)]
            return remote(spot, spot, xa_send.at[slot], xa_recv.at[slot], {"head": x_up})

        either(tile <= z, make, act)

    def down_copy(tile, slot, quarter, act):
        def make(count):
            spot = kv.at[tile, quarter, pl.ds(0, count)]
            return remote(spot, spot, xb_send.at[slot], xb_recv.at[slot], {"head": x_down})

        either(tile <= z, make, act)

    def across(tile, slot, q):
        if q == 0:
            up_copy(tile, slot, x, "start")
        else:
            down_copy(tile, slot, x_up, "start")

    def await_across(tile, slot):
        up_copy(tile, slot, x_down, "wait_recv")
        down_copy(tile, slot, lax.rem(x + 2, nx), "wait_recv")

    def pieces(values):
        for o in range(nx):
            for b in range(groups):
                yield b, o, values[(o * groups + b) * share:(o * groups + b + 1) * share]

    def latents():
        flat = normed[...].reshape(nx * mine, width)
        full = rms_scale(dot(flat, wl[...]), lgain)
        for b, o, v in pieces(full):
            pos = z * rows + o * share + lax.broadcasted_iota(jnp.int32, (share, 1), 0)
            lat[0, b, o * share:(o + 1) * share] = jnp.where(pos < lengths[b], v, 0.0)
        return full.astype(jnp.bfloat16).reshape(nx, mine, rank)

    def normed_of(k):
        o = lax.rem(x + k, nx)
        at = pl.ds(pl.multiple_of(o * share, share), share)
        raw = jnp.concatenate([hid[b, at].astype(jnp.float32) for b in range(groups)], axis=0)
        normed[o] = rms_scale(raw, gain).astype(jnp.bfloat16)

    def fill_own():
        ownlat[...] = latents()
        for k in range(2, nx):
            o = lax.rem(x + k, nx)
            kv[z, o] = ownlat[o]

    gain, lgain = small[:, :width], small[:, width:width + rank]
    for load in loads[:latent_at]:
        load.wait()
    lengths = [counts[0, b].astype(jnp.int32) for b in range(groups)]

    @pl.when(sec == 0)
    def _():
        normed_of(0)
        normed_of(1)

    for load in loads[latent_at:rest_at]:
        load.wait()
    for load in loads[rest_at:]:
        load.start()

    @pl.when(sec == 0)
    def _():
        rows_now = jnp.concatenate([normed[x], normed[x_up]], axis=0)
        early = rms_scale(dot(rows_now, wl[...]), lgain).astype(jnp.bfloat16)
        kv[z, x] = early[:mine]
        kv[z, x_up] = early[mine:]

    with jax.named_scope("barrier"):
        pl.semaphore_wait(barrier, len(peers))

    @pl.when(sec == 1)
    def _():
        for b in range(groups):
            with jax.named_scope("rswait"):
                for h in range(2):
                    for k in range(nx):
                        scatter_copy(b, h, x, k).wait_recv()
            at = pl.ds(b * share, share)
            own = hid[b, pl.ds(pl.multiple_of(x * share, share), share)].astype(jnp.float32)
            halves = []
            for h in range(2):
                add = headsum[0, b, h].astype(jnp.float32)
                for k in range(1, nx):
                    add = add + headsum[k, b, h].astype(jnp.float32)
                halves.append(own[:, h * half:(h + 1) * half] + add)
                xkeep[h, at] = halves[h]
            n = rms_scale(jnp.concatenate(halves, axis=1), gain)
            normed[x, at] = n.astype(jnp.bfloat16)
        early = rms_scale(dot(normed[x], wl[...]), lgain)
        kv[z, x] = early.astype(jnp.bfloat16)
        seed_copy(x).start()

    def first_sends(hop, q):
        right_copy(hop, hop, q, "start")
        left_copy(hop, hop, q, hop == 2, "start")

    @pl.when(sec == 0)
    def _():
        for hop in (2, 1):
            for q in range(2):
                first_sends(hop, q)

    @pl.when(sec == 1)
    def _():
        for hop in (2, 1):
            first_sends(hop, 0)
        for k in range(1, nx):
            normed_copy(lax.rem(x + k, nx), x).start()
        half_copy().start()
        with jax.named_scope("seedwait"):
            seed_copy(x_up).wait_recv()
        for hop in (2, 1):
            first_sends(hop, 1)

    def arrive(k):
        near, deep = 2 * k + 1, 2 * k + 2
        with jax.named_scope("zwait"):
            for q in range(2):
                right_copy(deep, 0, q, "wait_recv")

                @pl.when(k < levels - 1)
                def _():
                    right_copy(deep + 2, 2, q, "start")
                    left_copy(deep, 0, q, True, "wait_recv")

                @pl.when(k < levels - 2)
                def _():
                    left_copy(deep + 2, 2, q, True, "start")

            for q in range(2):

                @pl.when(k < levels - 1)
                def _():
                    right_copy(deep + 1, 1, q, "start")
                    left_copy(deep + 1, 1, q, False, "start")
                    across(tile_right(deep), mid + deep - 1, q)

                across(tile_left(deep), deep - 1, q)
            for q in range(2):
                right_copy(near, 0, q, "wait_recv")
                across(tile_left(near), near - 1, q)
                left_copy(near, 0, q, False, "wait_recv")
                across(tile_right(near), mid + near - 1, q)

    @pl.when(sec == 0)
    def _():
        with jax.named_scope("fill"):
            for k in range(2, nx):
                normed_of(k)
            fill_own()

    arrive(0)

    @pl.when(sec == 1)
    def _():
        with jax.named_scope("agwait"):
            for k in range(1, nx):
                normed_copy(x, lax.rem(x + k, nx)).wait_recv()
        fill_own()

    for load in loads[rest_at:rest_at + 2]:
        load.wait()
    with jax.named_scope("query"):
        query = dot(normed[...].reshape(nx * mine, width), wq[...]).astype(jnp.bfloat16)
        for h in range(heads):
            cols = slice(h * HD, (h + 1) * HD)
            a = (dot_t(query[:, cols], wk[:, cols]) * (1.0 / HD**0.5)).astype(jnp.bfloat16)
            for b, o, v in pieces(a):
                absorbed[b, h * rows + o * share:h * rows + (o + 1) * share] = v
        for b in range(groups):
            turned[b] = absorbed[b].T

    key_at = lax.broadcasted_iota(jnp.int32, (rows, hrows), 0)
    row_at = lax.broadcasted_iota(jnp.int32, (rows, hrows), 1) % rows

    def gather_keys(tiles):
        keys = []
        for b in range(groups):
            for t in tiles:
                keys.append(kv[t, :, b * share:(b + 1) * share].reshape(rows, rank))
        keys = jnp.concatenate(keys, axis=0)
        return keys, keys.T

    def fold(qb, scores, keys_t, tiles, own, light):
        parts = []
        each = rows * len(tiles)
        blocks = qb if light else qb + 1
        for b in range(blocks):
            for i, t in enumerate(tiles):
                start = b * each + i * rows
                s = scores[start:start + rows]
                if b < qb:
                    seen = key_at < lengths[b] - t * rows
                elif own:
                    seen = key_at <= row_at
                else:
                    seen = key_at < jnp.where(t < z, rows, 0)
                parts.append(jnp.where(seen, s, NEG))
        scores = jnp.concatenate(parts, axis=0)
        peak = jnp.max(scores, axis=0, keepdims=True)
        if not own:
            old = top[qb]
            peak = jnp.maximum(old, peak)
            shrink = jnp.exp(old - peak)
        weights = jnp.exp(scores - peak)
        add = jnp.sum(weights, axis=0, keepdims=True)
        gained = dot(keys_t, weights.astype(jnp.bfloat16))
        if own:
            total[qb] = add
            accum[qb] = gained
        else:
            total[qb] = total[qb] * shrink + add
            accum[qb] = accum[qb] * shrink + gained
        top[qb] = peak

    def attend(tiles, own, light):
        keys, keys_t = gather_keys(tiles)
        each = rows * len(tiles)

        def count(qb):
            return (qb if light else qb + 1) * each

        start = 1 if light else 0
        ahead = dot(keys[:count(start)], turned[start])
        for qb in range(start, groups):
            now = ahead
            if qb + 1 < groups:
                ahead = dot(keys[:count(qb + 1)], turned[qb + 1])
            fold(qb, now, keys_t[:, :count(qb)], tiles, own, light)

    with jax.named_scope("attend_own"):
        attend([z], True, False)

    def level(k, carry):
        arrive(k)

        def pair(d, c):
            with jax.named_scope("xwait"):
                await_across(tile_left(d), d - 1)
                await_across(tile_right(d), mid + d - 1)
            light = jnp.logical_and(z < d, z + d < nz)

            @pl.when(light)
            def _():
                with jax.named_scope("attend_light"):
                    attend([tile_left(d), tile_right(d)], False, True)

            @pl.when(jnp.logical_not(light))
            def _():
                with jax.named_scope("attend_pair"):
                    attend([tile_left(d), tile_right(d)], False, False)

            return c

        lax.fori_loop(2 * k - 1, 2 * k + 1, pair, 0)
        return carry

    lax.fori_loop(1, levels, level, 0)
    ends = [tile_left(mid - 1), tile_right(mid - 1), tile_left(mid)]
    with jax.named_scope("farwait"):
        await_across(ends[0], mid - 2)
        await_across(ends[1], 2 * mid - 2)
        await_across(ends[2], mid - 1)
    end_keys, end_turned = gather_keys(ends)
    last_keys[...] = end_keys
    last_turned[...] = end_turned
    all_later = z < mid - 1

    for load in loads[rest_at + 2:]:
        load.wait()

    def finish_copy(b, h, owner, source):
        return remote(
            part.at[b, owner, h], finsum.at[source, b], sum_send.at[b, h, owner], fin_recv.at[b, source],
            {"section": h, "head": owner},
        )

    for b in range(groups):

        def last_fold(light):
            n = (b if light else b + 1) * len(ends) * rows
            fold(b, dot(last_keys[:n], turned[b]), last_turned[:, :n], ends, False, light)

        with jax.named_scope("attend_last"):
            if b > 0:

                @pl.when(all_later)
                def _():
                    last_fold(True)

            @pl.when(jnp.logical_not(all_later))
            def _():
                last_fold(False)

        with jax.named_scope("project"):
            context = (accum[b] / total[b]).astype(jnp.bfloat16).T
            for h in range(heads):
                cols = slice(h * HD, (h + 1) * HD)
                attn[:, cols] = dot(context[h * rows:(h + 1) * rows], wv[:, cols]).astype(jnp.bfloat16)
        for h in range(2):
            with jax.named_scope("out"):
                out = dot(attn[...], wo[:, h * half:(h + 1) * half]).astype(jnp.bfloat16)
                for o in range(nx):
                    part[b, o, h] = out[o * share:(o + 1) * share]

            @pl.when(sec == 0)
            def _():
                for k in far_first + [0]:
                    scatter_copy(b, h, lax.rem(x + k, nx), x).start()

            @pl.when(sec == 1)
            def _():
                for k in far_first + [0] * (1 - h):
                    finish_copy(b, h, lax.rem(x + k, nx), x).start()

    def drain(k, carry):
        for d, hop in ((2 * k + 1, 1), (2 * k + 2, 2)):
            for q in range(2):
                right_copy(d, hop, q, "wait_send")
            up_copy(tile_left(d), d - 1, x, "wait_send")
            down_copy(tile_left(d), d - 1, x, "wait_send")

            @pl.when(d < mid)
            def _():
                for q in range(2):
                    left_copy(d, hop, q, hop == 2, "wait_send")
                up_copy(tile_right(d), mid + d - 1, x, "wait_send")
                down_copy(tile_right(d), mid + d - 1, x, "wait_send")

        return carry

    with jax.named_scope("drain"):
        lax.fori_loop(0, levels, drain, 0)

    @pl.when(sec == 0)
    def _():
        half_copy().wait_recv()
        for b in range(groups):
            for h in range(2):
                for o in range(nx):
                    scatter_copy(b, h, o, x).wait_send()

    @pl.when(sec == 1)
    def _():
        xhalf[...] = xkeep[1]
        half_copy().wait_send()
        seed_copy(x).wait_send()
        for k in range(1, nx):
            normed_copy(lax.rem(x + k, nx), x).wait_send()

    for b in range(groups):

        @pl.when(sec == 0)
        def _():
            with jax.named_scope("finwait0"):
                for k in range(nx):
                    finish_copy(b, 0, x, k).wait_recv()

        @pl.when(sec == 1)
        def _():
            finsum[x, b] = part[b, x, 1]
            with jax.named_scope("finwait1"):
                for k in range(1, nx):
                    finish_copy(b, 1, x, lax.rem(x + k, nx)).wait_recv()

        at = pl.ds(b * share, share)
        add = finsum[0, b].astype(jnp.float32)
        for k in range(1, nx):
            add = add + finsum[k, b].astype(jnp.float32)
        pos = z * rows + x * share + lax.broadcasted_iota(jnp.int32, (share, 1), 0)
        final[b] = jnp.where(pos < lengths[b], xhalf[at] + add, 0.0)

    @pl.when(sec == 1)
    def _():
        for b in range(groups):
            for k in range(1, nx):
                for h in range(2):
                    finish_copy(b, h, lax.rem(x + k, nx), x).wait_send()
            finish_copy(b, 0, x, x).wait_send()


def shards(nz, nx, hidden, lengths, attn_gain, w_query, w_latent, latent_gain, w_key, w_value, w_out):
    groups, rows, width = hidden.shape
    rank = w_latent.shape[2]
    cols = w_key.shape[2]
    heads = cols // HD
    share = rows // nx
    mine = groups * share
    half = width // 2
    mid = nz // 2
    vmem, dma = pltpu.VMEM, pltpu.SemaphoreType.DMA
    whole = pl.BlockSpec(memory_space=pltpu.VMEM)
    hbm = pl.BlockSpec(memory_space=pl.ANY)
    bf16, f32 = jnp.bfloat16, jnp.float32
    flat = ((0, 0, 0),)
    pieces = (attn_gain, latent_gain, lengths[None])
    size, at, small = width + rank + 128, 0, 0.0
    for piece in pieces:
        count = piece.shape[1]
        zero = jnp.zeros((), piece.dtype)
        small = small + lax.pad(piece, zero, flat + ((at, size - at - count, 0),)).astype(f32)
        at += count
    return pl.pallas_call(
        functools.partial(kernel, nz, nx),
        out_shape=(
            jax.ShapeDtypeStruct((groups, share, half), f32),
            jax.ShapeDtypeStruct((1, groups, rows, rank), f32),
        ),
        in_specs=[whole] + [hbm] * 6,
        out_specs=(whole, whole),
        scratch_shapes=[
            pltpu.SMEM((1, 128), f32),
            vmem((groups, rows, width), bf16),
            vmem((width, cols), bf16),
            vmem((width, rank), bf16),
            vmem((rank, cols), bf16),
            vmem((rank, cols), bf16),
            vmem((cols, width), bf16),
            vmem((nx, mine, width), bf16),
            vmem((nz, nx, mine, rank), bf16),
            vmem((nx, mine, rank), bf16),
            vmem((groups, heads * rows, rank), bf16),
            vmem((groups, rank, heads * rows), bf16),
            vmem((3 * groups * rows, rank), bf16),
            vmem((rank, 3 * groups * rows), bf16),
            vmem((groups, 1, heads * rows), f32),
            vmem((groups, 1, heads * rows), f32),
            vmem((groups, rank, heads * rows), f32),
            vmem((rows, cols), bf16),
            vmem((groups, nx, 2, share, half), bf16),
            vmem((nx, groups, 2, share, half), bf16),
            vmem((2, mine, half), f32),
            vmem((mine, half), f32),
            vmem((nx, groups, share, half), bf16),
            dma((groups + 9,)),
            dma((mid, 2)),
            dma((mid, 2)),
            dma((mid, 2)),
            dma((mid, 2)),
            dma((nz - 1,)),
            dma((nz - 1,)),
            dma((nz - 1,)),
            dma((nz - 1,)),
            dma,
            dma,
            dma((groups, 2, nx)),
            dma((groups, 2, nx)),
            dma((nx,)),
            dma((nx,)),
            dma,
            dma,
            dma((groups, nx)),
        ],
        compiler_params=pltpu.CompilerParams(
            collective_id=0, has_side_effects=True, vmem_limit_bytes=54500 * 1024
        ),
    )(small, hidden, w_query, w_latent, w_key, w_value, w_out)


def solution(mesh):
    return jax.shard_map(
        functools.partial(shards, mesh.shape["seq"], mesh.shape["head"]),
        mesh=mesh,
        in_specs=(
            P("rep", "seq", None),
            P("rep"),
            P("section", None),
            P("section", None, "head"),
            P("section", None, None),
            P("section", None),
            P("section", None, "head"),
            P("section", None, "head"),
            P("section", "head", None),
        ),
        out_specs=(P("rep", ("seq", "head"), "section"), P("section", "rep", "seq", None)),
        check_vma=False,
    )
```
